32 devices in a mesh: grp: 4 (over y, core), shard: 8 (over z, x).
Axes of the slice: x: 2, y: 2, z: 4, core: 2. Of those that a mesh axis runs over, the one named last changes fastest.
Arguments:
- grads: float32 [4, 8, 3456, 512], P('grp', 'shard'), may hold values from -6 to 6
- master: float32 [3456, 512], P('shard'), may hold values from -0.109375 to 0.109375
- moment_one: float32 [3456, 512], P('shard'), may hold values from -0.0004510549 to 0.0004510549
- moment_two: float32 [3456, 512], P('shard'), may hold values from 1.13028066e-10 to 2.8257017e-09
- step_count: int32 [1], replicated, may hold values from 1 to 59
Outputs:
- new_master: float32 [3456, 512], P('shard')
- new_moment_one: float32 [3456, 512], P('shard')
- new_moment_two: float32 [3456, 512], P('shard')
- weights: bfloat16 [3456, 512], replicated
The draws below stay inside these ranges and needn't reach their ends.
All inputs are finite; a program needn't handle non-finite values.
Results may differ from the reference program's by a relative error of at most 0.0004.
Values may be sent and summed in bfloat16 or wider, within the bound.
A program may use at most 128 MiB of HBM per device.

```python
import math
import jax
import jax.numpy as jnp
from jax import lax

IN = 3456
RANK = 512
N_GRP = 4
N_SHARD = 8


def strengthened(drawn, key, source, target, shards_of, factor):
    owner, partner = [(jnp.arange(drawn.shape[dim]) // (drawn.shape[dim] // shards_of)).reshape([-1 if axis == dim else 1 for axis in range(drawn.ndim)]) for dim in (source, target)]
    chosen = jax.random.permutation(key, shards_of)[partner]
    strong = (owner == chosen) | (owner == (partner + shards_of // 2) % shards_of)
    return jnp.where(strong, factor * drawn, drawn)


def shard_levels(key, dims, cuts, least, largest):
    loudness, own = 1.0, jax.random.fold_in(key, 6)
    for position, parts in cuts:
        steps = jnp.exp(jax.random.uniform(jax.random.fold_in(own, position), (parts,), jnp.float32, least / len(cuts), largest / len(cuts)))
        loudness = loudness * jnp.repeat(steps, dims[position] // parts).reshape([-1 if axis == position else 1 for axis in range(len(dims))])
    return loudness


def bell_draw(key, dims, deviation, reach, split=(), kind=jnp.bfloat16):
    result = deviation * jax.random.normal(key, dims, jnp.float32)
    if split:
        result = result * shard_levels(key, dims, split, -0.22, 0.18)
    return jnp.clip(result, -reach, reach).astype(kind)


def heavy_noise(rng, extent, deviation, reach, cuts, heavy, held_as=jnp.bfloat16):
    drawn = deviation * jax.random.normal(rng, extent, jnp.float32)
    if cuts:
        drawn = drawn * shard_levels(rng, extent, cuts, -0.22, 0.18)
    return jnp.clip(strengthened(drawn, jax.random.fold_in(rng, 3), *heavy), -reach, reach).astype(held_as)


def setup_inputs(seed: int = 0) -> dict:
    keys = jax.random.split(jax.random.key(seed), 6)
    grads = heavy_noise(keys[0], (N_GRP, N_SHARD, IN, RANK), 1.0, 6.0, ((0, 4), (1, 8)), (1, 2, 8, 2.0), jnp.float32)
    master = bell_draw(keys[1], (IN, RANK), IN ** -0.5, 0.109375, ((0, 8),), jnp.float32)
    moment_one = bell_draw(keys[2], (IN, RANK), (0.1 * (IN * RANK) ** -0.5), 0.0004510549, ((0, 8),), jnp.float32)
    moment_two = jnp.clip(jnp.exp(math.log(2.8257016726485062e-09) - 3.218876 * jax.random.uniform(keys[3], (IN, RANK), jnp.float32) ** shard_levels(keys[3], (IN, RANK), ((0, 8),), -0.2, 0.2)), 1.1302806607327298e-10, 2.8257016726485062e-09)
    step_count = jax.random.randint(keys[4], (1,), 1, 60).astype(jnp.int32)
    return dict(grads=grads, master=master, moment_one=moment_one, moment_two=moment_two, step_count=step_count)


def reference(grads, master, moment_one, moment_two, step_count):
    summed = lax.optimization_barrier(jnp.sum(grads, axis=(0, 1), dtype=jnp.float32))
    norm = jnp.sqrt(jnp.sum(summed * summed))
    clip = jnp.minimum(jnp.float32(1.0), 1.0 / (norm + 1e-06))
    gradient = clip * summed
    new_one = 0.9 * moment_one + 0.1 * gradient
    new_two = 0.999 * moment_two + 0.001 * gradient * gradient
    steps = step_count[0].astype(jnp.float32)
    first_fix = 1.0 - jnp.power(jnp.float32(0.9), steps)
    second_fix = 1.0 - jnp.power(jnp.float32(0.999), steps)
    update = new_one / first_fix / (jnp.sqrt(new_two / second_fix) + 1e-08)
    new_master = master - 0.01 * (update + 0.01 * master)
    return (new_master, new_one, new_two, new_master.astype(jnp.bfloat16))
```

```python
import functools
import jax
import jax.numpy as jnp
from jax import lax
from jax.experimental import pallas as pl
from jax.experimental.pallas import tpu as pltpu
from jax.sharding import PartitionSpec as P

MESH = pl.DeviceIdType.MESH
LANES = 128
TILE = 16
LEVELS = 32767.0
VMEM_LIMIT = 44 << 20

FLOWS = (
    (((1,), (0,), (2, 3)), 5),
    (((0,), (1,), (2, 3)), 5),
    (((2,), (3,), (0,), (1,)), 4),
    (((2,), (3,), (1,), (0,)), 3),
    (((1,), (0,), (2, 3)), 5),
    (((0,), (1,), (2, 3)), 5),
)


def flip(index, mask):
    bit = 1
    while bit <= mask:
        if mask & bit:
            index = index + bit * (1 - 2 * ((index // bit) % 2))
        bit *= 2
    return index


def bits_of(count):
    return count.bit_length() - 1


def split(tiles, weights):
    edges = [tiles * sum(weights[:i]) // sum(weights) for i in range(len(weights) + 1)]
    return [(low * TILE, (high - low) * TILE) for low, high in zip(edges, edges[1:])]


def reduce_order(stages):
    n = len(stages)
    order = [("ship", k, 0) for k in range(n)] + [("keep", k, -1) for k in range(n)]
    for s in range(1, max(len(x) for x in stages)):
        order += [("ship", k, s) for k in range(n) if s < len(stages[k])]
        order += [("keep", k, s - 1) for k in range(n) if s < len(stages[k])]
    return order


class Route:
    def __init__(self, stages, links):
        self.stages, self.links = stages, links
        self.radix = [1 << len(stage) for stage in stages]
        self.count = []
        below = 1
        for radix in reversed(self.radix):
            self.count.insert(0, below)
            below *= radix
        self.units = below
        self.base = [below - radix * count for radix, count in zip(self.radix, self.count)]
        self.last = len(stages) - 1

    def digit(self, unit, s):
        return unit // self.count[s] % self.radix[s]

    def mask(self, unit):
        a = b = 0
        for s, stage in enumerate(self.stages):
            digit = self.digit(unit, s)
            for i, link in enumerate(stage):
                if digit >> (len(stage) - 1 - i) & 1:
                    a, b = a ^ self.links[link][0], b ^ self.links[link][1]
        return a, b

    def stage_of(self, unit):
        return next((s for s in range(len(self.stages)) if self.digit(unit, s)), len(self.stages))

    def pieces(self, s):
        if s == self.last:
            return [(0, self.count[s])]
        return [(self.count[s + 1], self.count[s]), (0, self.count[s + 1])]


def kernel(n_grp, n_shard, links, routes, flows, *refs):
    refs = list(refs)
    n_flows, n_links = len(flows), len(links)
    steps_ref, grads, master, one, two = refs[:5]
    state = refs[5]
    gathered = refs[6:6 + n_flows]
    refs = refs[6 + n_flows:]
    acc, other, got, sbuf, rbuf, sscale, rscale, wown = (refs[i * n_flows:(i + 1) * n_flows] for i in range(8))
    (full, nown, nall, olds, news,
     lsem, csend, crecv, dsend, drecv, zsend, zrecv, gsend, grecv, nsend, nrecv,
     isem, osem, wsend, wrecv, lout, xsend, xrecv) = refs[8 * n_flows:]
    g, s_me = lax.axis_index("grp"), lax.axis_index("shard")
    rows, cols = master.shape
    core = g % 2

    grp_of = [flip(g, m) for m in range(n_grp)]
    shard_of = [flip(s_me, m) for m in range(n_shard)]
    lane_of = [pl.multiple_of(grp * LANES, LANES) for grp in grp_of]
    dims = list(range(bits_of(n_grp) - 2, -1, -1)) + list(range(n_links - 1, bits_of(n_grp) - 2, -1))
    bit = [g // links[l][0] % 2 if links[l][0] else s_me // links[l][1] % 2 for l in range(n_links)]

    def at(mask):
        return (grp_of[mask[0]], shard_of[mask[1]])

    def place(mask):
        return tuple(
            1 - bit[l] if (mask[0] & links[l][0]) or (mask[1] & links[l][1]) else bit[l] for l in dims)

    def columns(ref, gm):
        return ref.at[:, pl.ds(lane_of[gm], LANES)]

    mate = at((1, 0))
    barrier = pltpu.get_barrier_semaphore()
    peers = sorted({route.mask(d * route.count[s])
                    for route in routes for s in range(len(route.stages)) for d in range(1, route.radix[s])})
    near = [mate] + [at(m) for m in peers]
    for peer in near:
        pl.semaphore_signal(barrier, inc=1, device_id=peer, device_id_type=MESH)

    n_outer = grads.ndim - 2

    def fetch(k, target, parity, sem):
        offset, length = flows[k]
        for y in range(n_grp // 2):
            lanes = pl.ds(pl.multiple_of((2 * y + parity) * LANES, LANES), LANES)
            source = grads.at[(slice(None),) * n_outer + (pl.ds(offset, length), lanes)]
            head = tuple(y >> i & 1 for i in range(bits_of(n_grp) - 2, -1, -1))
            pltpu.make_async_copy(source, target[k].at[head], sem).start()

    def loaded(ref, sem):
        pltpu.make_async_copy(ref, ref, sem).wait()

    def cross(k, part):
        link = routes[k].stages[0][0]
        where = tuple((bit[l] if part == 0 else 1 - bit[l]) if l == link else slice(None) for l in dims)
        return pltpu.make_async_remote_copy(
            src_ref=other[k].at[where], dst_ref=got[k].at[where],
            send_sem=csend.at[k, part], recv_sem=crecv.at[k, part], device_id=mate, device_id_type=MESH)

    for k in range(n_flows):
        fetch(k, other, 1 - core, lsem.at[k, 1])
        fetch(k, acc, core, lsem.at[k, 0])
    pl.semaphore_wait(barrier, len(near))
    for k in range(n_flows):
        loaded(other[k], lsem.at[k, 1])
        cross(k, 1).start()
    for k in range(n_flows):
        cross(k, 0).start()

    grp_order = [0]
    for b in range(1, bits_of(n_grp)):
        grp_order = grp_order + [m ^ (1 << b) for m in grp_order]
    grp_order = grp_order + [m ^ 1 for m in grp_order]

    def whole(ref, send, recv):
        return pltpu.make_async_remote_copy(
            src_ref=ref, dst_ref=ref, send_sem=send, recv_sem=recv, device_id=mate, device_id_type=MESH)

    def message(k, s, d, p):
        route = routes[k]
        low, high = route.pieces(s)[p]
        start = route.base[s] + (d - 1) * route.count[s] + low
        span = pl.ds(start, high - low)
        to = at(route.mask(d * route.count[s]))
        return [
            pltpu.make_async_remote_copy(
                src_ref=sscale[k].at[span], dst_ref=rscale[k].at[span],
                send_sem=zsend.at[k, start], recv_sem=zrecv.at[k, start], device_id=to, device_id_type=MESH),
            pltpu.make_async_remote_copy(
                src_ref=sbuf[k].at[span], dst_ref=rbuf[k].at[span],
                send_sem=dsend.at[k, start], recv_sem=drecv.at[k, start], device_id=to, device_id_type=MESH),
        ]

    def await_piece(k, s, p):
        for d in range(1, routes[k].radix[s]):
            for copy in message(k, s, d, p):
                copy.wait_recv()

    def arrived(k, s, unit):
        route = routes[k]
        total = None
        for d in range(1, route.radix[s]):
            i = route.base[s] + (d - 1) * route.count[s] + unit
            value = rbuf[k][i].astype(jnp.int32).astype(jnp.float32) * rscale[k][i]
            total = value if total is None else total + value
        return total

    def ship(k, s):
        route, length = routes[k], flows[k][1]
        if s == 0:
            loaded(acc[k], lsem.at[k, 0])
            cross(k, 1).wait_recv()
        else:
            await_piece(k, s - 1, 0)
        count = route.count[s]
        for p, (low, high) in enumerate(route.pieces(s)):
            for d in range(1, route.radix[s]):
                for r in range(low, high):
                    unit = d * count + r
                    where = place(route.mask(unit))
                    value = acc[k][where] + (got[k][where] if s == 0 else arrived(k, s - 1, unit))
                    most = jnp.max(jnp.abs(value).reshape(length // 8, 8, LANES), axis=0)
                    top = jnp.maximum(jnp.max(most, axis=0, keepdims=True), 1e-30)
                    i = route.base[s] + (d - 1) * count + r
                    sscale[k][i] = top * (1.0 / LEVELS)
                    sbuf[k][i] = jnp.round(value * (LEVELS / top)).astype(jnp.int32).astype(jnp.int16)
                for copy in message(k, s, d, p):
                    copy.start()

    def keep(k, s):
        route = routes[k]
        if s < 0:
            cross(k, 0).wait_recv()
        else:
            await_piece(k, s, 1)
        for unit in range(route.count[s + 1]):
            where = place(route.mask(unit))
            acc[k][where] = acc[k][where] + (got[k][where] if s < 0 else arrived(k, s, unit))

    loads = []
    for kind, k, s in reduce_order([route.stages for route in routes]):
        if kind == "keep" and not loads:
            for n, source in enumerate((master, one, two)):
                for i, gm in enumerate(grp_order):
                    copy = pltpu.make_async_copy(columns(source, gm), olds.at[n, i], isem.at[n, i])
                    copy.start()
                    loads.append(copy)
        (ship if kind == "ship" else keep)(k, s)
    squares = jnp.zeros((8, LANES), jnp.float32)
    for k, (offset, length) in enumerate(flows):
        last = routes[k].last
        await_piece(k, last, 0)
        value = acc[k][place((0, 0))] + arrived(k, last, 0)
        full[0, offset:offset + length] = value
        squares = squares + jnp.sum((value * value).reshape(length // 8, 8, LANES), axis=0)
    nown[...] = jnp.sum(squares, axis=0, keepdims=True)
    me = g * n_shard + s_me
    everyone = n_grp * n_shard

    def tell(gm, sm):
        return pltpu.make_async_remote_copy(
            src_ref=nown, dst_ref=nall.at[me], send_sem=nsend, recv_sem=nrecv,
            device_id=at((gm, sm)), device_id_type=MESH)

    for gm in range(n_grp):
        for sm in range(n_shard):
            if gm or sm:
                tell(gm, sm).start()
    nall[me] = nown[...]

    def share(n, mask, index):
        return pltpu.make_async_remote_copy(
            src_ref=full.at[pl.ds(0, n)], dst_ref=full.at[pl.ds(n, n)],
            send_sem=gsend.at[index], recv_sem=grecv.at[index], device_id=at((mask, 0)), device_id_type=MESH)

    shares = []
    for index in range(bits_of(n_grp)):
        mask = 1 if index == bits_of(n_grp) - 1 else 2 << index
        shares.append(share(1 << index, mask, index))
    for index in range(len(shares) - 1):
        shares[index].start()
        if index < len(shares) - 2:
            shares[index].wait_recv()

    for copy in loads:
        copy.wait()
    t = jnp.full((8, LANES), steps_ref[0], jnp.int32).astype(jnp.float32)
    first_fix = (1.0 - jnp.power(jnp.full((8, LANES), 0.9, jnp.float32), t))[0:1]
    second_fix = (1.0 - jnp.power(jnp.full((8, LANES), 0.999, jnp.float32), t))[0:1]
    others = nall.at[pl.ds(0, everyone - 1)]
    whole(others, nsend, nrecv).wait()
    norm = jnp.sqrt(jnp.sum(jnp.sum(nall[...], axis=0), axis=1, keepdims=True))
    clip = jnp.minimum(1.0, 1.0 / (norm + 1e-6))

    def update(i, k):
        offset, length = flows[k]
        tiles = length // TILE
        group = max(d for d in range(1, 6) if tiles % d == 0) * TILE

        def body(r, carry):
            span = pl.ds(pl.multiple_of(offset + r * group, TILE), group)
            gradient = clip * full[i, span]
            m_one = 0.9 * olds[1, i, span] + 0.1 * gradient
            m_two = 0.999 * olds[2, i, span] + 0.001 * gradient * gradient
            step = m_one / first_fix / (jnp.sqrt(m_two / second_fix) + 1e-8)
            old = olds[0, i, span]
            fresh = old - 0.01 * (step + 0.01 * old)
            news[0, i, span] = fresh
            news[1, i, span] = m_one
            news[2, i, span] = m_two
            if i == 0:
                wown[k][pl.ds(pl.multiple_of(r * group, TILE), group)] = fresh.astype(jnp.bfloat16)
            return carry

        lax.fori_loop(0, length // group, body, 0)

    def slot(k, unit):
        return gathered[k].at[(core,) + place(routes[k].mask(unit))]

    def push(k, unit, s, d):
        route = routes[k]
        lands = unit + d * route.count[s]
        return pltpu.make_async_remote_copy(
            src_ref=slot(k, unit) if unit else wown[k], dst_ref=slot(k, unit),
            send_sem=wsend.at[k, lands], recv_sem=wrecv.at[k, lands],
            device_id=at(route.mask(d * route.count[s])), device_id_type=MESH)

    def forward(k, unit):
        route = routes[k]
        for s in range(route.stage_of(unit) - 1, -1, -1):
            for d in range(1, route.radix[s]):
                push(k, unit, s, d).start()
        pltpu.make_async_remote_copy(
            src_ref=slot(k, unit) if unit else wown[k], dst_ref=slot(k, unit),
            send_sem=xsend.at[k], recv_sem=xrecv.at[k], device_id=mate, device_id_type=MESH).start()
        if unit == 0:
            pltpu.make_async_copy(wown[k], slot(k, 0), lout.at[k]).start()

    def arrive(k, unit):
        route = routes[k]
        s = route.stage_of(unit)
        d = route.digit(unit, s)
        push(k, unit - d * route.count[s], s, d).wait_recv()
        forward(k, unit)

    stores = []

    def states(low, high):
        for i in range(low, high):
            if i:
                for k in range(n_flows):
                    update(i, k)
            for n in range(3):
                copy = pltpu.make_async_copy(
                    news.at[n, i], columns(state.at[n], grp_order[i]), osem.at[n, i])
                copy.start()
                stores.append(copy)

    for k in range(n_flows):
        update(0, k)
        forward(k, 0)
    if len(shares) > 1:
        shares[-2].wait_recv()
    shares[-1].start()
    half = len(grp_order) // 2
    states(0, half)
    depth = max(len(route.stages) for route in routes)
    for t in range(depth):
        for k, route in enumerate(routes):
            for unit in range(1, route.units):
                if route.last - route.stage_of(unit) == t:
                    arrive(k, unit)
        if t == 0:
            shares[-1].wait_recv()
            states(half, len(grp_order))

    for k, route in enumerate(routes):
        for part in (0, 1):
            cross(k, part).wait_send()
        for s in range(len(route.stages)):
            for d in range(1, route.radix[s]):
                for p in range(len(route.pieces(s))):
                    for copy in message(k, s, d, p):
                        copy.wait_send()
    for copy in shares:
        copy.wait_send()
    for k, route in enumerate(routes):
        for unit in range(1, route.units):
            s = route.stage_of(unit)
            d = route.digit(unit, s)
            push(k, unit - d * route.count[s], s, d).wait_send()
        pltpu.make_async_copy(wown[k], slot(k, 0), lout.at[k]).wait()
    for copy in stores:
        copy.wait()
    for k in range(n_flows):
        whole(gathered[k].at[1 - core], xsend.at[k], xrecv.at[k]).wait()


def place_out(flows, n_outer, *refs):
    n_flows = len(flows)
    state, gathered = refs[0], refs[1:1 + n_flows]
    outs, weights, sem = refs[1 + n_flows:4 + n_flows], refs[4 + n_flows], refs[5 + n_flows]
    copies = []
    for k, (offset, length) in enumerate(flows):
        n_head = gathered[k].ndim - 2 - n_outer
        for i in range(1 << n_head):
            head = tuple(i >> b & 1 for b in range(n_head))
            grp = sum(h << b for b, h in enumerate(head))
            where = (slice(None),) * n_outer + (pl.ds(offset, length), pl.ds(grp * LANES, LANES))
            head = head[:1] + head[:0:-1]
            copies.append(pltpu.make_async_copy(gathered[k].at[head], weights.at[where], sem.at[len(copies)]))
    for n in range(3):
        copies.append(pltpu.make_async_copy(state.at[n], outs[n], sem.at[len(copies)]))
    for copy in copies:
        copy.start()
    for copy in copies:
        copy.wait()


def fused(mesh, grads, master, moment_one, moment_two, step_count):
    n_grp, n_shard = mesh.shape["grp"], mesh.shape["shard"]
    rows, cols = master.shape
    links = [(2 << i, 0) for i in range(bits_of(n_grp) - 1)] + [(0, 1 << i) for i in range(bits_of(n_shard))]
    n_links, n_units = len(links), 1 << len(links)
    routes = [Route(stages, links) for stages, _ in FLOWS]
    flows = split(rows // TILE, [weight for _, weight in FLOWS])
    n_flows, n_outer = len(flows), bits_of(n_shard)
    vmem, dma = pltpu.VMEM, pltpu.SemaphoreType.DMA
    any_space, hbm_space = pl.BlockSpec(memory_space=pl.ANY), pl.BlockSpec(memory_space=pltpu.HBM)
    n_share = bits_of(n_grp)
    cube = (2,) * n_links
    scratch = []
    for _ in range(3):
        scratch += [vmem(cube + (length, LANES), jnp.float32) for _, length in flows]
    for _ in range(2):
        scratch += [vmem((n_units - 1, length, LANES), jnp.int16) for _, length in flows]
    for _ in range(2):
        scratch += [vmem((n_units - 1, 1, LANES), jnp.float32) for _ in flows]
    scratch += [vmem((length, LANES), jnp.bfloat16) for _, length in flows]
    scratch += [
        vmem((n_grp, rows, LANES), jnp.float32),
        vmem((1, LANES), jnp.float32),
        vmem((n_grp * n_shard, 1, LANES), jnp.float32),
        vmem((3, n_grp, rows, LANES), jnp.float32),
        vmem((3, n_grp, rows, LANES), jnp.float32),
        dma((n_flows, 2)), dma((n_flows, 2)), dma((n_flows, 2)),
        dma((n_flows, n_units)), dma((n_flows, n_units)), dma((n_flows, n_units)), dma((n_flows, n_units)),
        dma((n_share,)), dma((n_share,)), dma, dma,
        dma((3, n_grp)), dma((3, n_grp)),
        dma((n_flows, n_units)), dma((n_flows, n_units)), dma((n_flows,)), dma((n_flows,)), dma((n_flows,)),
    ]
    cut = (2,) * n_outer + (rows, cols)
    state, *gathered = pl.pallas_call(
        functools.partial(kernel, n_grp, n_shard, links, routes, flows),
        out_shape=[jax.ShapeDtypeStruct((3, rows, cols), jnp.float32)] + [
            jax.ShapeDtypeStruct((2,) + cube + (length, LANES), jnp.bfloat16) for _, length in flows],
        in_specs=[pl.BlockSpec(memory_space=pltpu.SMEM)] + [hbm_space] * 4,
        out_specs=[any_space] * (1 + n_flows),
        scratch_shapes=scratch,
        compiler_params=pltpu.CompilerParams(collective_id=0, has_side_effects=True, vmem_limit_bytes=VMEM_LIMIT),
    )(step_count, *(pltpu.with_memory_space_constraint(x, pltpu.HBM)
                    for x in (grads[0, 0].reshape(cut), master, moment_one, moment_two)))
    *outs, weights = pl.pallas_call(
        functools.partial(place_out, flows, n_outer),
        out_shape=[jax.ShapeDtypeStruct((rows, cols), jnp.float32)] * 3 + [jax.ShapeDtypeStruct(cut, jnp.bfloat16)],
        in_specs=[any_space] * (1 + n_flows),
        out_specs=[hbm_space] * 4,
        scratch_shapes=[dma((3 + n_flows * n_grp,))],
        compiler_params=pltpu.CompilerParams(vmem_limit_bytes=1 << 20),
    )(state, *gathered)
    return (*outs, weights.reshape(rows * n_shard, cols))


def plain(grads, master, moment_one, moment_two, step_count):
    local = grads[0, 0]
    count = master.shape[0]
    total = lax.psum(local, ("grp", "shard"))
    squares = jnp.sum(total * total)
    start = lax.axis_index("shard") * count
    gradient = lax.dynamic_slice_in_dim(total, start, count, 0)
    norm = jnp.sqrt(squares)
    clip = jnp.minimum(jnp.float32(1.0), 1.0 / (norm + 1e-06))
    gradient = clip * gradient
    new_one = 0.9 * moment_one + 0.1 * gradient
    new_two = 0.999 * moment_two + 0.001 * gradient * gradient
    steps = step_count[0].astype(jnp.float32)
    first_fix = 1.0 - jnp.power(jnp.float32(0.9), steps)
    second_fix = 1.0 - jnp.power(jnp.float32(0.999), steps)
    update = new_one / first_fix / (jnp.sqrt(new_two / second_fix) + 1e-08)
    new_master = master - 0.01 * (update + 0.01 * master)
    weights = lax.all_gather(new_master.astype(jnp.bfloat16), "shard", axis=0, tiled=True)
    return (new_master, new_one, new_two, weights)


def solution(mesh):
    n_grp, n_shard = mesh.shape["grp"], mesh.shape["shard"]

    def shards(grads, master, moment_one, moment_two, step_count):
        rows, cols = master.shape
        powers = all(n & (n - 1) == 0 for n in (n_grp, n_shard))
        links = bits_of(n_grp) - 1 + bits_of(n_shard)
        matched = {link for stages, _ in FLOWS for stage in stages for link in stage} == set(range(links))
        if powers and n_grp > 2 and matched and cols == LANES * n_grp and rows % TILE == 0:
            return fused(mesh, grads, master, moment_one, moment_two, step_count)
        return plain(grads, master, moment_one, moment_two, step_count)

    return jax.shard_map(
        shards,
        mesh=mesh,
        in_specs=(
            P("grp", "shard", None, None),
            P("shard", None),
            P("shard", None),
            P("shard", None),
            P(),
        ),
        out_specs=(P("shard", None), P("shard", None), P("shard", None), P()),
        check_vma=False,
    )
```

```python
import functools
import jax
import jax.numpy as jnp
from jax import lax
from jax.experimental import pallas as pl
from jax.experimental.pallas import tpu as pltpu
from jax.sharding import PartitionSpec as P

MESH = pl.DeviceIdType.MESH
LANES = 128
TILE = 16
LEVELS = 32767.0
VMEM_LIMIT = 44 << 20

FLOWS = (
    (((1,), (0,), (2, 3)), 6),
    (((0,), (1,), (2, 3)), 6),
    (((2,), (3,), (0, 1)), 6),
    (((1,), (0,), (2, 3)), 5),
    (((0,), (1,), (2, 3)), 4),
)


def flip(index, mask):
    bit = 1
    while bit <= mask:
        if mask & bit:
            index = index + bit * (1 - 2 * ((index // bit) % 2))
        bit *= 2
    return index


def bits_of(count):
    return count.bit_length() - 1


def split(tiles, weights):
    edges = [tiles * sum(weights[:i]) // sum(weights) for i in range(len(weights) + 1)]
    return [(low * TILE, (high - low) * TILE) for low, high in zip(edges, edges[1:])]


def reduce_order(stages):
    n = len(stages)
    order = [("ship", k, 0) for k in range(n)] + [("keep", k, -1) for k in range(n)]
    for s in range(1, max(len(x) for x in stages)):
        order += [("ship", k, s) for k in range(n) if s < len(stages[k])]
        order += [("keep", k, s - 1) for k in range(n) if s < len(stages[k])]
    return order


def gather_order(routes):
    order = []
    for step in range(max(len(route.stages) for route in routes)):
        for k, route in enumerate(routes):
            t = route.last - step
            if t >= 0:
                order += [(k, t, origin) for origin in sorted(route.groups(t), reverse=True)]
    return order


class Route:
    def __init__(self, stages, links):
        self.stages, self.links = stages, links
        self.radix = [1 << len(stage) for stage in stages]
        self.count = []
        below = 1
        for radix in reversed(self.radix):
            self.count.insert(0, below)
            below *= radix
        self.units = below
        self.base = [below - radix * count for radix, count in zip(self.radix, self.count)]
        self.last = len(stages) - 1

    def digit(self, unit, s):
        return unit // self.count[s] % self.radix[s]

    def mask(self, unit):
        a = b = 0
        for s, stage in enumerate(self.stages):
            digit = self.digit(unit, s)
            for i, link in enumerate(stage):
                if digit >> (len(stage) - 1 - i) & 1:
                    a, b = a ^ self.links[link][0], b ^ self.links[link][1]
        return a, b

    def stage_of(self, unit):
        return next((s for s in range(len(self.stages)) if self.digit(unit, s)), len(self.stages))

    def pieces(self, s):
        if s == self.last:
            return [(0, self.count[s])]
        return [(self.count[s + 1], self.count[s]), (0, self.count[s + 1])]

    def groups(self, t):
        found = {}
        for d in range(1, self.radix[t]):
            for unit in range(self.count[t]):
                found.setdefault(self.stage_of(unit), []).append((unit, d))
        return found


def numbered(routes):
    pieces, groups = {}, {}
    for k, route in enumerate(routes):
        for s in range(len(route.stages)):
            for p in range(len(route.pieces(s))):
                pieces[k, s, p] = len(pieces)
            for t in route.groups(s):
                groups[k, s, t] = len(groups)
    return pieces, groups


def kernel(n_grp, n_shard, links, routes, flows, *refs):
    refs = list(refs)
    n_flows, n_links = len(flows), len(links)
    steps_ref, grads, master, one, two = refs[:5]
    state = refs[5]
    gathered = refs[6:6 + n_flows]
    refs = refs[6 + n_flows:]
    acc, got, sbuf, rbuf, sscale, rscale, wown = (refs[i * n_flows:(i + 1) * n_flows] for i in range(7))
    (full, nown, nall, olds, news, meter,
     lsem, csend, crecv, send, recv, gsend, grecv, nsend, nrecv,
     isem, osem, wsend, wrecv, lout, xsend, xrecv) = refs[7 * n_flows:]
    pieces, groups = numbered(routes)
    g, s_me = lax.axis_index("grp"), lax.axis_index("shard")
    rows, cols = master.shape
    core = g % 2

    grp_of = [flip(g, m) for m in range(n_grp)]
    shard_of = [flip(s_me, m) for m in range(n_shard)]
    lane_of = [pl.multiple_of(grp * LANES, LANES) for grp in grp_of]
    dims = list(range(bits_of(n_grp) - 2, -1, -1)) + list(range(n_links - 1, bits_of(n_grp) - 2, -1))
    bit = [g // links[l][0] % 2 if links[l][0] else s_me // links[l][1] % 2 for l in range(n_links)]

    def at(mask):
        return (grp_of[mask[0]], shard_of[mask[1]])

    def place(mask):
        return tuple(
            1 - bit[l] if (mask[0] & links[l][0]) or (mask[1] & links[l][1]) else bit[l] for l in dims)

    def columns(ref, gm):
        return ref.at[:, pl.ds(lane_of[gm], LANES)]

    mate = at((1, 0))
    barrier = pltpu.get_barrier_semaphore()
    peers = sorted({route.mask(d * route.count[s])
                    for route in routes for s in range(len(route.stages)) for d in range(1, route.radix[s])})
    near = [mate] + [at(m) for m in peers]
    for peer in near:
        pl.semaphore_signal(barrier, inc=1, device_id=peer, device_id_type=MESH)

    n_outer = grads.ndim - 2

    def parts(k, part, parity):
        offset, length = flows[k]
        link = routes[k].stages[0][0]
        where = tuple((bit[l] if part == 0 else 1 - bit[l]) if l == link else slice(None) for l in dims)
        head, outer = where[:len(dims) - n_outer], where[len(dims) - n_outer:]
        if any(isinstance(h, slice) for h in head):
            heads = [tuple(y >> i & 1 for i in range(len(head) - 1, -1, -1)) for y in range(1 << len(head))]
        else:
            heads = [head]
        for h in heads:
            grp = sum(b << (len(h) - 1 - i) for i, b in enumerate(h))
            lanes = pl.ds(pl.multiple_of((2 * grp + parity) * LANES, LANES), LANES)
            yield grads.at[outer + (pl.ds(offset, length), lanes)], h + outer

    def cube_part(ref, k, part):
        link = routes[k].stages[0][0]
        return ref.at[tuple((bit[l] if part == 0 else 1 - bit[l]) if l == link else slice(None) for l in dims)]

    def fetch(k, part):
        for source, where in parts(k, part, core):
            pltpu.make_async_copy(source, acc[k].at[where], lsem.at[k, part]).start()

    def cross(k, part):
        for source, where in parts(k, part, 1 - core):
            pltpu.make_async_remote_copy(
                src_ref=source, dst_ref=got[k].at[where],
                send_sem=csend, recv_sem=crecv.at[k, part],
                device_id=mate, device_id_type=MESH).start()

    def crossed(k, part):
        ref = cube_part(got[k], k, part)
        return pltpu.make_async_remote_copy(
            src_ref=ref, dst_ref=ref, send_sem=csend, recv_sem=crecv.at[k, part],
            device_id=mate, device_id_type=MESH)

    def loaded(k, part):
        ref = cube_part(acc[k], k, part)
        pltpu.make_async_copy(ref, ref, lsem.at[k, part]).wait()

    for k in range(n_flows):
        fetch(k, 1)
    pl.semaphore_wait(barrier, len(near))
    for k in range(n_flows):
        cross(k, 1)
    for k in range(n_flows):
        fetch(k, 0)
        cross(k, 0)

    grp_order = [0]
    for b in range(1, bits_of(n_grp)):
        grp_order = grp_order + [m ^ (1 << b) for m in grp_order]
    grp_order = grp_order + [m ^ 1 for m in grp_order]

    def whole(ref, send, recv):
        return pltpu.make_async_remote_copy(
            src_ref=ref, dst_ref=ref, send_sem=send, recv_sem=recv, device_id=mate, device_id_type=MESH)

    def message(k, s, d, p):
        route = routes[k]
        low, high = route.pieces(s)[p]
        start = route.base[s] + (d - 1) * route.count[s] + low
        span = pl.ds(start, high - low)
        to = at(route.mask(d * route.count[s]))
        return [
            pltpu.make_async_remote_copy(
                src_ref=sscale[k].at[span], dst_ref=rscale[k].at[span],
                send_sem=send, recv_sem=recv.at[pieces[k, s, p]], device_id=to, device_id_type=MESH),
            pltpu.make_async_remote_copy(
                src_ref=sbuf[k].at[span], dst_ref=rbuf[k].at[span],
                send_sem=send, recv_sem=recv.at[pieces[k, s, p]], device_id=to, device_id_type=MESH),
        ]

    def rows_of(k, units):
        return units * flows[k][1] // 2

    def metered(n, send_sem, recv_sem):
        return whole(meter.at[pl.ds(0, n)], send_sem, recv_sem)

    def await_piece(k, s, p):
        low, high = routes[k].pieces(s)[p]
        units = (routes[k].radix[s] - 1) * (high - low)
        metered(rows_of(k, units) + units, send, recv.at[pieces[k, s, p]]).wait_recv()

    def arrived(k, s, unit):
        route = routes[k]
        total = None
        for d in range(1, route.radix[s]):
            i = route.base[s] + (d - 1) * route.count[s] + unit
            value = rbuf[k][i].astype(jnp.int32).astype(jnp.float32) * rscale[k][i]
            total = value if total is None else total + value
        return total

    def ship(k, s):
        route, length = routes[k], flows[k][1]
        if s == 0:
            loaded(k, 1)
            crossed(k, 1).wait_recv()
        else:
            await_piece(k, s - 1, 0)
        count = route.count[s]
        for p, (low, high) in enumerate(route.pieces(s)):
            for d in range(1, route.radix[s]):
                for r in range(low, high):
                    unit = d * count + r
                    where = place(route.mask(unit))
                    value = acc[k][where] + (got[k][where] if s == 0 else arrived(k, s - 1, unit))
                    most = jnp.max(jnp.abs(value).reshape(length // 8, 8, LANES), axis=0)
                    top = jnp.maximum(jnp.max(most, axis=0, keepdims=True), 1e-30)
                    i = route.base[s] + (d - 1) * count + r
                    sscale[k][i] = top * (1.0 / LEVELS)
                    sbuf[k][i] = jnp.round(value * (LEVELS / top)).astype(jnp.int32).astype(jnp.int16)
                for copy in message(k, s, d, p):
                    copy.start()

    def keep(k, s):
        route = routes[k]
        if s < 0:
            loaded(k, 0)
            crossed(k, 0).wait_recv()
        else:
            await_piece(k, s, 1)
        for unit in range(route.count[s + 1]):
            where = place(route.mask(unit))
            acc[k][where] = acc[k][where] + (got[k][where] if s < 0 else arrived(k, s, unit))

    loading = False
    for kind, k, s in reduce_order([route.stages for route in routes]):
        if kind == "keep" and not loading:
            loading = True
            for n, source in enumerate((master, one, two)):
                for i, gm in enumerate(grp_order):
                    pltpu.make_async_copy(columns(source, gm), olds.at[n, i], isem).start()
        (ship if kind == "ship" else keep)(k, s)
    squares = jnp.zeros((8, LANES), jnp.float32)
    for k, (offset, length) in enumerate(flows):
        last = routes[k].last
        await_piece(k, last, 0)
        value = acc[k][place((0, 0))] + arrived(k, last, 0)
        full[0, offset:offset + length] = value
        squares = squares + jnp.sum((value * value).reshape(length // 8, 8, LANES), axis=0)
    nown[...] = jnp.sum(squares, axis=0, keepdims=True)
    me = g * n_shard + s_me
    everyone = n_grp * n_shard

    def tell(gm, sm):
        return pltpu.make_async_remote_copy(
            src_ref=nown, dst_ref=nall.at[me], send_sem=nsend, recv_sem=nrecv,
            device_id=at((gm, sm)), device_id_type=MESH)

    for gm in range(n_grp):
        for sm in range(n_shard):
            if gm or sm:
                tell(gm, sm).start()
    nall[me] = nown[...]

    def share(n, mask, index):
        return pltpu.make_async_remote_copy(
            src_ref=full.at[pl.ds(0, n)], dst_ref=full.at[pl.ds(n, n)],
            send_sem=gsend.at[index], recv_sem=grecv.at[index], device_id=at((mask, 0)), device_id_type=MESH)

    shares = []
    for index in range(bits_of(n_grp)):
        mask = 1 if index == bits_of(n_grp) - 1 else 2 << index
        shares.append(share(1 << index, mask, index))
    for index in range(len(shares) - 1):
        shares[index].start()
        if index < len(shares) - 2:
            shares[index].wait_recv()

    pltpu.make_async_copy(olds, olds, isem).wait()
    t = jnp.full((8, LANES), steps_ref[0], jnp.int32).astype(jnp.float32)
    first_fix = (1.0 - jnp.power(jnp.full((8, LANES), 0.9, jnp.float32), t))[0:1]
    second_fix = (1.0 - jnp.power(jnp.full((8, LANES), 0.999, jnp.float32), t))[0:1]
    others = nall.at[pl.ds(0, everyone - 1)]
    whole(others, nsend, nrecv).wait()
    norm = jnp.sqrt(jnp.sum(jnp.sum(nall[...], axis=0), axis=1, keepdims=True))
    clip = jnp.minimum(1.0, 1.0 / (norm + 1e-6))

    def update(i, k):
        offset, length = flows[k]
        tiles = length // TILE
        group = max(d for d in range(1, 6) if tiles % d == 0) * TILE

        def body(r, carry):
            span = pl.ds(pl.multiple_of(offset + r * group, TILE), group)
            gradient = clip * full[i, span]
            m_one = 0.9 * olds[1, i, span] + 0.1 * gradient
            m_two = 0.999 * olds[2, i, span] + 0.001 * gradient * gradient
            step = m_one / first_fix / (jnp.sqrt(m_two / second_fix) + 1e-8)
            old = olds[0, i, span]
            fresh = old - 0.01 * (step + 0.01 * old)
            news[0, i, span] = fresh
            news[1, i, span] = m_one
            news[2, i, span] = m_two
            if i == 0:
                wown[k][pl.ds(pl.multiple_of(r * group, TILE), group)] = fresh.astype(jnp.bfloat16)
            return carry

        lax.fori_loop(0, length // group, body, 0)

    def slot(k, unit):
        return gathered[k].at[(core,) + place(routes[k].mask(unit))]

    def push(k, unit, s, d):
        route = routes[k]
        return pltpu.make_async_remote_copy(
            src_ref=slot(k, unit) if unit else wown[k], dst_ref=slot(k, unit),
            send_sem=wsend, recv_sem=wrecv.at[groups[k, s, route.stage_of(unit)]],
            device_id=at(route.mask(d * route.count[s])), device_id_type=MESH)

    def forward(k, unit):
        route = routes[k]
        for s in range(route.stage_of(unit) - 1, -1, -1):
            for d in range(1, route.radix[s]):
                push(k, unit, s, d).start()
        pltpu.make_async_remote_copy(
            src_ref=slot(k, unit) if unit else wown[k], dst_ref=slot(k, unit),
            send_sem=xsend, recv_sem=xrecv, device_id=mate, device_id_type=MESH).start()
        if unit == 0:
            pltpu.make_async_copy(wown[k], slot(k, 0), lout).start()

    def arrive(k, t, origin):
        route = routes[k]
        members = route.groups(t)[origin]
        metered(rows_of(k, len(members)), wsend, wrecv.at[groups[k, t, origin]]).wait_recv()
        for unit, d in members:
            forward(k, unit + d * route.count[t])


    def states(low, high):
        for i in range(low, high):
            if i:
                for k in range(n_flows):
                    update(i, k)
            for n in range(3):
                pltpu.make_async_copy(news.at[n, i], columns(state.at[n], grp_order[i]), osem).start()

    for k in range(n_flows):
        update(0, k)
        forward(k, 0)
    if len(shares) > 1:
        shares[-2].wait_recv()
    shares[-1].start()
    half = len(grp_order) // 2
    states(0, half)
    for index, (k, t, origin) in enumerate(gather_order(routes)):
        if index == n_flows:
            shares[-1].wait_recv()
            states(half, len(grp_order))
        arrive(k, t, origin)

    n_units = routes[0].units
    others = sum(rows_of(k, n_units - 1) for k in range(n_flows))
    metered(4 * sum(rows_of(k, n_units) for k in range(n_flows)) // 2, csend, nrecv).wait_send()
    metered(others + n_flows * (n_units - 1), send, nrecv).wait_send()
    metered(others, wsend, nrecv).wait_send()
    for copy in shares:
        copy.wait_send()
    own = meter.at[pl.ds(0, sum(rows_of(k, 1) for k in range(n_flows)))]
    pltpu.make_async_copy(own, own, lout).wait()
    pltpu.make_async_copy(news, news, osem).wait()
    metered(sum(rows_of(k, n_units) for k in range(n_flows)), xsend, xrecv).wait()


def place_out(flows, n_outer, *refs):
    n_flows = len(flows)
    state, gathered = refs[0], refs[1:1 + n_flows]
    outs, weights, outs_sem, weights_sem = refs[1 + n_flows:4 + n_flows], *refs[4 + n_flows:]
    for k, (offset, length) in enumerate(flows):
        n_head = gathered[k].ndim - 2 - n_outer
        for i in range(1 << n_head):
            head = tuple(i >> b & 1 for b in range(n_head))
            grp = sum(h << b for b, h in enumerate(head))
            where = (slice(None),) * n_outer + (pl.ds(offset, length), pl.ds(grp * LANES, LANES))
            head = head[:1] + head[:0:-1]
            pltpu.make_async_copy(gathered[k].at[head], weights.at[where], weights_sem).start()
    for n in range(3):
        pltpu.make_async_copy(state.at[n], outs[n], outs_sem).start()
    pltpu.make_async_copy(state, state, outs_sem).wait()
    pltpu.make_async_copy(weights, weights, weights_sem).wait()


def fused(mesh, grads, master, moment_one, moment_two, step_count):
    n_grp, n_shard = mesh.shape["grp"], mesh.shape["shard"]
    rows, cols = master.shape
    links = [(2 << i, 0) for i in range(bits_of(n_grp) - 1)] + [(0, 1 << i) for i in range(bits_of(n_shard))]
    n_links, n_units = len(links), 1 << len(links)
    routes = [Route(stages, links) for stages, _ in FLOWS]
    flows = split(rows // TILE, [weight for _, weight in FLOWS])
    n_flows, n_outer = len(flows), bits_of(n_shard)
    vmem, dma = pltpu.VMEM, pltpu.SemaphoreType.DMA
    any_space, hbm_space = pl.BlockSpec(memory_space=pl.ANY), pl.BlockSpec(memory_space=pltpu.HBM)
    n_share = bits_of(n_grp)
    pieces, groups = numbered(routes)
    cube = (2,) * n_links
    scratch = []
    for _ in range(2):
        scratch += [vmem(cube + (length, LANES), jnp.float32) for _, length in flows]
    for _ in range(2):
        scratch += [vmem((n_units - 1, length, LANES), jnp.int16) for _, length in flows]
    for _ in range(2):
        scratch += [vmem((n_units - 1, 1, LANES), jnp.float32) for _ in flows]
    scratch += [vmem((length, LANES), jnp.bfloat16) for _, length in flows]
    scratch += [
        vmem((n_grp, rows, LANES), jnp.float32),
        vmem((1, LANES), jnp.float32),
        vmem((n_grp * n_shard, 1, LANES), jnp.float32),
        vmem((3, n_grp, rows, LANES), jnp.float32),
        vmem((3, n_grp, rows, LANES), jnp.float32),
        vmem((n_units * rows, 1, LANES), jnp.float32),
        dma((n_flows, 2)), dma, dma((n_flows, 2)), dma, dma((len(pieces),)),
        dma((n_share,)), dma((n_share,)), dma, dma,
        dma, dma, dma, dma((len(groups),)), dma, dma, dma,
    ]
    cut = (2,) * n_outer + (rows, cols)
    state, *gathered = pl.pallas_call(
        functools.partial(kernel, n_grp, n_shard, links, routes, flows),
        out_shape=[jax.ShapeDtypeStruct((3, rows, cols), jnp.float32)] + [
            jax.ShapeDtypeStruct((2,) + cube + (length, LANES), jnp.bfloat16) for _, length in flows],
        in_specs=[pl.BlockSpec(memory_space=pltpu.SMEM)] + [hbm_space] * 4,
        out_specs=[any_space] * (1 + n_flows),
        scratch_shapes=scratch,
        compiler_params=pltpu.CompilerParams(collective_id=0, has_side_effects=True, vmem_limit_bytes=VMEM_LIMIT),
    )(step_count, *(pltpu.with_memory_space_constraint(x, pltpu.HBM)
                    for x in (grads[0, 0].reshape(cut), master, moment_one, moment_two)))
    *outs, weights = pl.pallas_call(
        functools.partial(place_out, flows, n_outer),
        out_shape=[jax.ShapeDtypeStruct((rows, cols), jnp.float32)] * 3 + [jax.ShapeDtypeStruct(cut, jnp.bfloat16)],
        in_specs=[any_space] * (1 + n_flows),
        out_specs=[hbm_space] * 4,
        scratch_shapes=[dma, dma],
        compiler_params=pltpu.CompilerParams(vmem_limit_bytes=1 << 20),
    )(state, *gathered)
    return (*outs, weights.reshape(rows * n_shard, cols))


def plain(grads, master, moment_one, moment_two, step_count):
    local = grads[0, 0]
    count = master.shape[0]
    total = lax.psum(local, ("grp", "shard"))
    squares = jnp.sum(total * total)
    start = lax.axis_index("shard") * count
    gradient = lax.dynamic_slice_in_dim(total, start, count, 0)
    norm = jnp.sqrt(squares)
    clip = jnp.minimum(jnp.float32(1.0), 1.0 / (norm + 1e-06))
    gradient = clip * gradient
    new_one = 0.9 * moment_one + 0.1 * gradient
    new_two = 0.999 * moment_two + 0.001 * gradient * gradient
    steps = step_count[0].astype(jnp.float32)
    first_fix = 1.0 - jnp.power(jnp.float32(0.9), steps)
    second_fix = 1.0 - jnp.power(jnp.float32(0.999), steps)
    update = new_one / first_fix / (jnp.sqrt(new_two / second_fix) + 1e-08)
    new_master = master - 0.01 * (update + 0.01 * master)
    weights = lax.all_gather(new_master.astype(jnp.bfloat16), "shard", axis=0, tiled=True)
    return (new_master, new_one, new_two, weights)


def solution(mesh):
    n_grp, n_shard = mesh.shape["grp"], mesh.shape["shard"]

    def shards(grads, master, moment_one, moment_two, step_count):
        rows, cols = master.shape
        powers = all(n & (n - 1) == 0 for n in (n_grp, n_shard))
        links = bits_of(n_grp) - 1 + bits_of(n_shard)
        matched = {link for stages, _ in FLOWS for stage in stages for link in stage} == set(range(links))
        if powers and n_grp > 2 and matched and cols == LANES * n_grp and rows % TILE == 0:
            return fused(mesh, grads, master, moment_one, moment_two, step_count)
        return plain(grads, master, moment_one, moment_two, step_count)

    return jax.shard_map(
        shards,
        mesh=mesh,
        in_specs=(
            P("grp", "shard", None, None),
            P("shard", None),
            P("shard", None),
            P("shard", None),
            P(),
        ),
        out_specs=(P("shard", None), P("shard", None), P("shard", None), P()),
        check_vma=False,
    )
```

```python
import functools
import jax
import jax.numpy as jnp
from jax import lax
from jax.experimental import pallas as pl
from jax.experimental.pallas import tpu as pltpu
from jax.sharding import PartitionSpec as P

MESH = pl.DeviceIdType.MESH
LANES = 128
TILE = 16
LEVELS = 32767.0
VMEM_LIMIT = 44 << 20

REDUCE = (
    (((2,), (0,), (1,), (3,)), 3),
    (((0,), (1,), (2, 3)), 4),
    (((0,), (1,), (3,), (2,)), 5),
    (((1,), (3,), (2, 0)), 5),
    (((2,), (0,), (1,), (3,)), 8),
    (((1,), (0,), (2, 3)), 2),
)
SHIP, KEEP, FINISH = range(3)
REDUCE_STEPS = (
    (0, 0, 0), (0, 1, 0), (0, 2, 0), (0, 3, 0), (0, 4, 0), (0, 5, 0), (1, 0, -1), (1, 1, -1),
    (1, 2, -1), (0, 0, 1), (1, 3, -1), (0, 1, 1), (1, 0, 0), (1, 4, -1), (1, 5, -1), (0, 3, 1),
    (1, 1, 0), (1, 3, 0), (0, 2, 1), (0, 4, 1), (0, 5, 1), (1, 5, 0), (1, 2, 0), (0, 0, 2),
    (0, 1, 2), (1, 1, 1), (1, 0, 1), (0, 2, 2), (1, 4, 0), (0, 4, 2), (1, 2, 1), (0, 3, 2),
    (0, 0, 3), (1, 3, 1), (1, 0, 2), (1, 4, 1), (0, 5, 2), (1, 5, 1), (2, 1, 0), (0, 4, 3),
    (0, 2, 3), (1, 4, 2), (1, 2, 2), (2, 0, 0), (2, 3, 0), (2, 5, 0), (2, 2, 0), (2, 4, 0),
)
GATHER = (
    (((0,), (1,), (2,), (3,)), 7),
    (((0,), (2,), (1,), (3,)), 8),
    (((1,), (2,), (0,), (3,)), 6),
    (((2,), (0, 1), (3,)), 6),
)
GATHER_STEPS = (
    (0, 1, 4), (0, 0, 4), (1, 2, 4), (1, 0, 4), (0, 2, 4), (0, 3, 4), (2, 0, 4), (2, 2, 4),
    (1, 1, 4), (3, 1, 3), (1, 3, 4), (2, 1, 4), (2, 3, 4), (0, 1, 3), (3, 0, 3), (0, 0, 3),
    (3, 2, 3), (0, 2, 3), (1, 2, 3), (1, 0, 3), (2, 0, 3), (2, 2, 3), (1, 1, 3), (2, 1, 3),
    (3, 1, 2), (0, 1, 2), (3, 0, 2), (0, 0, 2), (1, 0, 2), (1, 1, 2), (2, 0, 2), (2, 1, 2),
    (0, 0, 1), (3, 0, 1), (1, 0, 1), (2, 0, 1),
)
SHARE_AT, STATES_AT = (4, (0, 6, 9, 12))


def flip(index, mask):
    bit = 1
    while bit <= mask:
        if mask & bit:
            index = index + bit * (1 - 2 * ((index // bit) % 2))
        bit *= 2
    return index


def bits_of(count):
    return count.bit_length() - 1


def split(tiles, weights):
    edges = [tiles * sum(weights[:i]) // sum(weights) for i in range(len(weights) + 1)]
    return [(low * TILE, (high - low) * TILE) for low, high in zip(edges, edges[1:])]


class Route:
    def __init__(self, stages, links):
        self.stages, self.links = stages, links
        self.radix = [1 << len(stage) for stage in stages]
        self.count = []
        below = 1
        for radix in reversed(self.radix):
            self.count.insert(0, below)
            below *= radix
        self.units = below
        self.base = [below - radix * count for radix, count in zip(self.radix, self.count)]
        self.last = len(stages) - 1

    def digit(self, unit, s):
        return unit // self.count[s] % self.radix[s]

    def mask(self, unit):
        a = b = 0
        for s, stage in enumerate(self.stages):
            digit = self.digit(unit, s)
            for i, link in enumerate(stage):
                if digit >> (len(stage) - 1 - i) & 1:
                    a, b = a ^ self.links[link][0], b ^ self.links[link][1]
        return a, b

    def stage_of(self, unit):
        return next((s for s in range(len(self.stages)) if self.digit(unit, s)), len(self.stages))

    def pieces(self, s):
        if s == self.last:
            return [(0, self.count[s])]
        return [(self.count[s + 1], self.count[s]), (0, self.count[s + 1])]

    def groups(self, t):
        found = {}
        for d in range(1, self.radix[t]):
            for unit in range(self.count[t]):
                found.setdefault(self.stage_of(unit), []).append((unit, d))
        return found


def numbered(routes, part):
    keys = [(k, s, p) for k, route in enumerate(routes) for s in range(len(route.stages)) for p in part(route, s)]
    return {key: i for i, key in enumerate(keys)}


def numbered_pieces(routes):
    return numbered(routes, lambda route, s: range(len(route.pieces(s))))


def numbered_groups(routes):
    return numbered(routes, Route.groups)


def kernel(n_grp, n_shard, links, reduction, gather, *refs):
    refs = list(refs)
    (routes, flows), (g_routes, g_flows) = reduction, gather
    n_flows, n_gather, n_links = len(flows), len(g_flows), len(links)

    def take(count):
        taken = refs[:count]
        del refs[:count]
        return taken

    count_ref, grads, master, one, two, state = take(6)
    gathered = take(n_gather)
    acc, got, sbuf, rbuf, sscale, rscale = (take(n_flows) for _ in range(6))
    wown = take(n_gather)
    (full, nown, nall, olds, news, meter, steps_ref,
     sems, csend, send, gsend, grecv, nsend, nrecv,
     isem, osem, wsend, lout, xsend, xrecv, tsem) = refs
    pieces, groups = numbered_pieces(routes), numbered_groups(g_routes)
    g, s_me = lax.axis_index("grp"), lax.axis_index("shard")
    rows, cols = master.shape
    core = g % 2

    grp_of = [flip(g, m) for m in range(n_grp)]
    shard_of = [flip(s_me, m) for m in range(n_shard)]
    lane_of = [pl.multiple_of(grp * LANES, LANES) for grp in grp_of]
    dims = list(range(bits_of(n_grp) - 2, -1, -1)) + list(range(n_links - 1, bits_of(n_grp) - 2, -1))
    bit = [g // links[l][0] % 2 if links[l][0] else s_me // links[l][1] % 2 for l in range(n_links)]

    def at(mask):
        return (grp_of[mask[0]], shard_of[mask[1]])

    def place(mask):
        return tuple(
            1 - bit[l] if (mask[0] & links[l][0]) or (mask[1] & links[l][1]) else bit[l] for l in dims)

    def columns(ref, gm):
        return ref.at[:, pl.ds(lane_of[gm], LANES)]

    mate = at((1, 0))
    barrier = pltpu.get_barrier_semaphore()
    peers = sorted({route.mask(d * route.count[s])
                    for route in routes + g_routes for s in range(len(route.stages)) for d in range(1, route.radix[s])})
    pltpu.make_async_copy(count_ref, steps_ref, tsem).start()
    near = [mate] + [at(m) for m in peers]
    for peer in near:
        pl.semaphore_signal(barrier, inc=1, device_id=peer, device_id_type=MESH)

    n_outer = grads.ndim - 2

    def parts(k, part, parity):
        offset, length = flows[k]
        link = routes[k].stages[0][0]
        where = tuple((bit[l] if part == 0 else 1 - bit[l]) if l == link else slice(None) for l in dims)
        head, outer = where[:len(dims) - n_outer], where[len(dims) - n_outer:]
        if any(isinstance(h, slice) for h in head):
            heads = [tuple(y >> i & 1 for i in range(len(head) - 1, -1, -1)) for y in range(1 << len(head))]
        else:
            heads = [head]
        for h in heads:
            grp = sum(b << (len(h) - 1 - i) for i, b in enumerate(h))
            lanes = pl.ds(pl.multiple_of((2 * grp + parity) * LANES, LANES), LANES)
            yield grads.at[outer + (pl.ds(offset, length), lanes)], h + outer

    def cube_part(ref, k, part):
        link = routes[k].stages[0][0]
        return ref.at[tuple((bit[l] if part == 0 else 1 - bit[l]) if l == link else slice(None) for l in dims)]

    def fetch(k, part):
        for source, where in parts(k, part, core):
            pltpu.make_async_copy(source, acc[k].at[where], sems.at[2 * k + part]).start()

    def cross(k, part):
        for source, where in parts(k, part, 1 - core):
            pltpu.make_async_remote_copy(
                src_ref=source, dst_ref=got[k].at[where],
                send_sem=csend, recv_sem=sems.at[2 * (n_flows + k) + part],
                device_id=mate, device_id_type=MESH).start()

    def crossed(k, part):
        ref = cube_part(got[k], k, part)
        return pltpu.make_async_remote_copy(
            src_ref=ref, dst_ref=ref, send_sem=csend, recv_sem=sems.at[2 * (n_flows + k) + part],
            device_id=mate, device_id_type=MESH)

    def loaded(k, part):
        ref = cube_part(acc[k], k, part)
        pltpu.make_async_copy(ref, ref, sems.at[2 * k + part]).wait()

    for k in range(n_flows):
        fetch(k, 1)
    pl.semaphore_wait(barrier, len(near))
    for k in range(n_flows):
        cross(k, 1)
    for k in range(n_flows):
        fetch(k, 0)
        cross(k, 0)

    grp_order = [0]
    for b in range(1, bits_of(n_grp)):
        grp_order = grp_order + [m ^ (1 << b) for m in grp_order]
    grp_order = grp_order + [m ^ 1 for m in grp_order]

    def whole(ref, send, recv):
        return pltpu.make_async_remote_copy(
            src_ref=ref, dst_ref=ref, send_sem=send, recv_sem=recv, device_id=mate, device_id_type=MESH)

    def message(k, s, d, p):
        route = routes[k]
        low, high = route.pieces(s)[p]
        start = route.base[s] + (d - 1) * route.count[s] + low
        span = pl.ds(start, high - low)
        to = at(route.mask(d * route.count[s]))
        return [
            pltpu.make_async_remote_copy(
                src_ref=sscale[k].at[span], dst_ref=rscale[k].at[span],
                send_sem=send, recv_sem=sems.at[4 * n_flows + pieces[k, s, p]], device_id=to, device_id_type=MESH),
            pltpu.make_async_remote_copy(
                src_ref=sbuf[k].at[span], dst_ref=rbuf[k].at[span],
                send_sem=send, recv_sem=sems.at[4 * n_flows + pieces[k, s, p]], device_id=to, device_id_type=MESH),
        ]

    def rows_of(units, length):
        return units * length // 2

    def metered(n, send_sem, recv_sem):
        return whole(meter.at[pl.ds(0, n)], send_sem, recv_sem)

    def await_piece(k, s, p):
        low, high = routes[k].pieces(s)[p]
        units = (routes[k].radix[s] - 1) * (high - low)
        metered(rows_of(units, flows[k][1]) + units, send, sems.at[4 * n_flows + pieces[k, s, p]]).wait_recv()

    def arrived(k, s, unit):
        route = routes[k]
        total = None
        for d in range(1, route.radix[s]):
            i = route.base[s] + (d - 1) * route.count[s] + unit
            value = rbuf[k][i].astype(jnp.int32).astype(jnp.float32) * rscale[k][i]
            total = value if total is None else total + value
        return total

    def ship(k, s):
        route, length = routes[k], flows[k][1]
        if s == 0:
            loaded(k, 1)
            crossed(k, 1).wait_recv()
        else:
            await_piece(k, s - 1, 0)
        count = route.count[s]
        for p, (low, high) in enumerate(route.pieces(s)):
            for d in range(1, route.radix[s]):
                for r in range(low, high):
                    unit = d * count + r
                    where = place(route.mask(unit))
                    value = acc[k][where] + (got[k][where] if s == 0 else arrived(k, s - 1, unit))
                    most = jnp.max(jnp.abs(value).reshape(length // 8, 8, LANES), axis=0)
                    top = jnp.maximum(jnp.max(most, axis=0, keepdims=True), 1e-30)
                    i = route.base[s] + (d - 1) * count + r
                    sscale[k][i] = top * (1.0 / LEVELS)
                    sbuf[k][i] = jnp.round(value * (LEVELS / top)).astype(jnp.int32).astype(jnp.int16)
                for copy in message(k, s, d, p):
                    copy.start()

    def keep(k, s):
        route = routes[k]
        if s < 0:
            loaded(k, 0)
            crossed(k, 0).wait_recv()
        else:
            await_piece(k, s, 1)
        for unit in range(route.count[s + 1]):
            where = place(route.mask(unit))
            acc[k][where] = acc[k][where] + (got[k][where] if s < 0 else arrived(k, s, unit))

    def load_state():
        for n, source in enumerate((master, one, two)):
            for i, gm in enumerate(grp_order):
                pltpu.make_async_copy(columns(source, gm), olds.at[n, i], isem).start()

    def finish(k):
        offset, length = flows[k]
        last = routes[k].last
        await_piece(k, last, 0)
        value = acc[k][place((0, 0))] + arrived(k, last, 0)
        full[0, offset:offset + length] = value
        return jnp.sum((value * value).reshape(length // 8, 8, LANES), axis=0)

    squares = jnp.zeros((8, LANES), jnp.float32)
    for index, (kind, k, s) in enumerate(REDUCE_STEPS):
        if index == n_flows:
            load_state()
        if kind == SHIP:
            ship(k, s)
        elif kind == KEEP:
            keep(k, s)
        else:
            squares = squares + finish(k)
    nown[...] = jnp.sum(squares, axis=0, keepdims=True)
    me = g * n_shard + s_me
    everyone = n_grp * n_shard

    def tell(gm, sm):
        return pltpu.make_async_remote_copy(
            src_ref=nown, dst_ref=nall.at[me], send_sem=nsend, recv_sem=nrecv,
            device_id=at((gm, sm)), device_id_type=MESH)

    for gm in range(n_grp):
        for sm in range(n_shard):
            if gm or sm:
                tell(gm, sm).start()
    nall[me] = nown[...]

    def share(n, mask, index):
        return pltpu.make_async_remote_copy(
            src_ref=full.at[pl.ds(0, n)], dst_ref=full.at[pl.ds(n, n)],
            send_sem=gsend.at[index], recv_sem=grecv.at[index], device_id=at((mask, 0)), device_id_type=MESH)

    shares = []
    for index in range(bits_of(n_grp)):
        mask = 1 if index == bits_of(n_grp) - 1 else 2 << index
        shares.append(share(1 << index, mask, index))
    for index in range(len(shares) - 1):
        shares[index].start()
        if index < len(shares) - 2:
            shares[index].wait_recv()

    pltpu.make_async_copy(olds, olds, isem).wait()
    pltpu.make_async_copy(count_ref, steps_ref, tsem).wait()
    t = jnp.full((8, LANES), steps_ref[0], jnp.int32).astype(jnp.float32)
    first_fix = (1.0 - jnp.power(jnp.full((8, LANES), 0.9, jnp.float32), t))[0:1]
    second_fix = (1.0 - jnp.power(jnp.full((8, LANES), 0.999, jnp.float32), t))[0:1]
    others = nall.at[pl.ds(0, everyone - 1)]
    whole(others, nsend, nrecv).wait()
    norm = jnp.sqrt(jnp.sum(jnp.sum(nall[...], axis=0), axis=1, keepdims=True))
    clip = jnp.minimum(1.0, 1.0 / (norm + 1e-6))

    def update(i, k):
        offset, length = g_flows[k]
        tiles = length // TILE
        group = max(d for d in range(1, 6) if tiles % d == 0) * TILE

        def body(r, carry):
            span = pl.ds(pl.multiple_of(offset + r * group, TILE), group)
            gradient = clip * full[i, span]
            m_one = 0.9 * olds[1, i, span] + 0.1 * gradient
            m_two = 0.999 * olds[2, i, span] + 0.001 * gradient * gradient
            step = m_one / first_fix / (jnp.sqrt(m_two / second_fix) + 1e-8)
            old = olds[0, i, span]
            fresh = old - 0.01 * (step + 0.01 * old)
            news[0, i, span] = fresh
            news[1, i, span] = m_one
            news[2, i, span] = m_two
            if i == 0:
                wown[k][pl.ds(pl.multiple_of(r * group, TILE), group)] = fresh.astype(jnp.bfloat16)
            return carry

        lax.fori_loop(0, length // group, body, 0)

    def slot(k, unit):
        return gathered[k].at[(core,) + place(g_routes[k].mask(unit))]

    def push(k, unit, s, d):
        route = g_routes[k]
        return pltpu.make_async_remote_copy(
            src_ref=slot(k, unit) if unit else wown[k], dst_ref=slot(k, unit),
            send_sem=wsend, recv_sem=sems.at[groups[k, s, route.stage_of(unit)]],
            device_id=at(route.mask(d * route.count[s])), device_id_type=MESH)

    def forward(k, unit):
        route = g_routes[k]
        for s in range(route.stage_of(unit) - 1, -1, -1):
            for d in range(1, route.radix[s]):
                push(k, unit, s, d).start()
        pltpu.make_async_remote_copy(
            src_ref=slot(k, unit) if unit else wown[k], dst_ref=slot(k, unit),
            send_sem=xsend, recv_sem=xrecv, device_id=mate, device_id_type=MESH).start()
        if unit == 0:
            pltpu.make_async_copy(wown[k], slot(k, 0), lout).start()

    def arrive(k, t, origin):
        route = g_routes[k]
        members = route.groups(t)[origin]
        metered(rows_of(len(members), g_flows[k][1]), wsend, sems.at[groups[k, t, origin]]).wait_recv()
        for unit, d in members:
            forward(k, unit + d * route.count[t])


    def share_on():
        if len(shares) > 1:
            shares[-2].wait_recv()
        shares[-1].start()

    def states(i):
        if i == len(grp_order) // 2:
            shares[-1].wait_recv()
        if i:
            for k in range(n_gather):
                update(i, k)
        for n in range(3):
            pltpu.make_async_copy(news.at[n, i], columns(state.at[n], grp_order[i]), osem).start()

    for k in range(n_gather):
        update(0, k)
        forward(k, 0)
    for index in range(len(GATHER_STEPS) + 1):
        if index == SHARE_AT:
            share_on()
        for i, when in enumerate(STATES_AT):
            if index == when:
                states(i)
        if index < len(GATHER_STEPS):
            arrive(*GATHER_STEPS[index])

    n_units = routes[0].units
    metered(n_units * rows, csend, nrecv).wait_send()
    metered(rows_of(n_units - 1, rows) + n_flows * (n_units - 1), send, nrecv).wait_send()
    metered(rows_of(n_units - 1, rows), wsend, nrecv).wait_send()
    for copy in shares:
        copy.wait_send()
    own = meter.at[pl.ds(0, rows // 2)]
    pltpu.make_async_copy(own, own, lout).wait()
    pltpu.make_async_copy(news, news, osem).wait()
    metered(rows_of(n_units, rows), xsend, xrecv).wait()


def place_out(flows, n_outer, *refs):
    n_flows = len(flows)
    state, gathered = refs[0], refs[1:1 + n_flows]
    outs, weights, outs_sem, weights_sem = refs[1 + n_flows:4 + n_flows], *refs[4 + n_flows:]
    for k, (offset, length) in enumerate(flows):
        n_head = gathered[k].ndim - 2 - n_outer
        for i in range(1 << n_head):
            head = tuple(i >> b & 1 for b in range(n_head))
            grp = sum(h << b for b, h in enumerate(head))
            where = (slice(None),) * n_outer + (pl.ds(offset, length), pl.ds(grp * LANES, LANES))
            head = head[:1] + head[:0:-1]
            pltpu.make_async_copy(gathered[k].at[head], weights.at[where], weights_sem).start()
    for n in range(3):
        pltpu.make_async_copy(state.at[n], outs[n], outs_sem).start()
    pltpu.make_async_copy(state, state, outs_sem).wait()
    pltpu.make_async_copy(weights, weights, weights_sem).wait()


def fused(mesh, grads, master, moment_one, moment_two, step_count):
    n_grp, n_shard = mesh.shape["grp"], mesh.shape["shard"]
    rows, cols = master.shape
    links = [(2 << i, 0) for i in range(bits_of(n_grp) - 1)] + [(0, 1 << i) for i in range(bits_of(n_shard))]
    n_links, n_units = len(links), 1 << len(links)
    reduction, gather = (
        ([Route(stages, links) for stages, _ in entries], split(rows // TILE, [weight for _, weight in entries]))
        for entries in (REDUCE, GATHER))
    flows, g_flows = reduction[1], gather[1]
    n_flows, n_gather, n_outer = len(flows), len(g_flows), bits_of(n_shard)
    vmem, dma = pltpu.VMEM, pltpu.SemaphoreType.DMA
    any_space, hbm_space = pl.BlockSpec(memory_space=pl.ANY), pl.BlockSpec(memory_space=pltpu.HBM)
    n_share = bits_of(n_grp)
    n_pieces, n_groups = len(numbered_pieces(reduction[0])), len(numbered_groups(gather[0]))
    cube = (2,) * n_links
    scratch = []
    for _ in range(2):
        scratch += [vmem(cube + (length, LANES), jnp.float32) for _, length in flows]
    for _ in range(2):
        scratch += [vmem((n_units - 1, length, LANES), jnp.int16) for _, length in flows]
    for _ in range(2):
        scratch += [vmem((n_units - 1, 1, LANES), jnp.float32) for _ in flows]
    scratch += [vmem((length, LANES), jnp.bfloat16) for _, length in g_flows]
    scratch += [
        vmem((n_grp, rows, LANES), jnp.float32),
        vmem((1, LANES), jnp.float32),
        vmem((n_grp * n_shard, 1, LANES), jnp.float32),
        vmem((3, n_grp, rows, LANES), jnp.float32),
        vmem((3, n_grp, rows, LANES), jnp.float32),
        vmem((n_units * rows, 1, LANES), jnp.float32),
        pltpu.SMEM((1,), jnp.int32),
        dma((max(4 * n_flows + n_pieces, n_groups),)), dma, dma, dma((n_share,)), dma((n_share,)), dma, dma,
        dma, dma, dma, dma, dma, dma, dma,
    ]
    cut = (2,) * n_outer + (rows, cols)
    state, *gathered = pl.pallas_call(
        functools.partial(kernel, n_grp, n_shard, links, reduction, gather),
        out_shape=[jax.ShapeDtypeStruct((3, rows, cols), jnp.float32)] + [
            jax.ShapeDtypeStruct((2,) + cube + (length, LANES), jnp.bfloat16) for _, length in g_flows],
        in_specs=[any_space] + [hbm_space] * 4,
        out_specs=[any_space] * (1 + n_gather),
        scratch_shapes=scratch,
        compiler_params=pltpu.CompilerParams(collective_id=0, has_side_effects=True, vmem_limit_bytes=VMEM_LIMIT),
    )(step_count, *(pltpu.with_memory_space_constraint(x, pltpu.HBM)
                    for x in (grads[0, 0].reshape(cut), master, moment_one, moment_two)))
    *outs, weights = pl.pallas_call(
        functools.partial(place_out, g_flows, n_outer),
        out_shape=[jax.ShapeDtypeStruct((rows, cols), jnp.float32)] * 3 + [jax.ShapeDtypeStruct(cut, jnp.bfloat16)],
        in_specs=[any_space] * (1 + n_gather),
        out_specs=[hbm_space] * 4,
        scratch_shapes=[dma, dma],
        compiler_params=pltpu.CompilerParams(vmem_limit_bytes=1 << 20),
    )(state, *gathered)
    return (*outs, weights.reshape(rows * n_shard, cols))


def plain(grads, master, moment_one, moment_two, step_count):
    local = grads[0, 0]
    count = master.shape[0]
    total = lax.psum(local, ("grp", "shard"))
    squares = jnp.sum(total * total)
    start = lax.axis_index("shard") * count
    gradient = lax.dynamic_slice_in_dim(total, start, count, 0)
    norm = jnp.sqrt(squares)
    clip = jnp.minimum(jnp.float32(1.0), 1.0 / (norm + 1e-06))
    gradient = clip * gradient
    new_one = 0.9 * moment_one + 0.1 * gradient
    new_two = 0.999 * moment_two + 0.001 * gradient * gradient
    steps = step_count[0].astype(jnp.float32)
    first_fix = 1.0 - jnp.power(jnp.float32(0.9), steps)
    second_fix = 1.0 - jnp.power(jnp.float32(0.999), steps)
    update = new_one / first_fix / (jnp.sqrt(new_two / second_fix) + 1e-08)
    new_master = master - 0.01 * (update + 0.01 * master)
    weights = lax.all_gather(new_master.astype(jnp.bfloat16), "shard", axis=0, tiled=True)
    return (new_master, new_one, new_two, weights)


def solution(mesh):
    n_grp, n_shard = mesh.shape["grp"], mesh.shape["shard"]

    def shards(grads, master, moment_one, moment_two, step_count):
        rows, cols = master.shape
        powers = all(n & (n - 1) == 0 for n in (n_grp, n_shard))
        links = bits_of(n_grp) - 1 + bits_of(n_shard)
        matched = {link for stages, _ in REDUCE for stage in stages for link in stage} == set(range(links))
        if powers and n_grp > 2 and matched and cols == LANES * n_grp and rows % TILE == 0:
            return fused(mesh, grads, master, moment_one, moment_two, step_count)
        return plain(grads, master, moment_one, moment_two, step_count)

    return jax.shard_map(
        shards,
        mesh=mesh,
        in_specs=(
            P("grp", "shard", None, None),
            P("shard", None),
            P("shard", None),
            P("shard", None),
            P(),
        ),
        out_specs=(P("shard", None), P("shard", None), P("shard", None), P()),
        check_vma=False,
    )
```

```python
import functools
import jax
import jax.numpy as jnp
from jax import lax
from jax.experimental import pallas as pl
from jax.experimental.pallas import tpu as pltpu
from jax.sharding import PartitionSpec as P

MESH = pl.DeviceIdType.MESH
LANES = 128
TILE = 16
LEVELS = 32767.0
VMEM_LIMIT = 44 << 20

REDUCE = (
    (((2,), (0,), (1,), (3,)), 3),
    (((0,), (1,), (2, 3)), 4),
    (((0,), (1,), (3,), (2,)), 5),
    (((1,), (3,), (2, 0)), 5),
    (((2,), (0,), (1,), (3,)), 8),
    (((1,), (0,), (2, 3)), 2),
)
REDUCE_STEPS = (
    (0, 0, 0), (1, 0, 0), (2, 0, 0), (3, 0, 0), (0, 0, 1), (4, 0, 0), (1, 0, 1), (5, 0, 0),
    (2, 0, 1), (0, 1, 0), (3, 0, 1), (1, 1, 0), (0, 0, 2), (4, 0, 1), (3, 1, 0), (1, 0, 2),
    (5, 0, 1), (2, 1, 0), (2, 0, 2), (0, 1, 1), (4, 1, 0), (3, 0, 2), (0, 0, 3), (1, 1, 1),
    (5, 1, 0), (4, 0, 2), (3, 1, 1), (0, 2, 0), (5, 0, 2), (2, 0, 3), (2, 1, 1), (1, 2, 0),
    (0, 1, 2), (4, 1, 1), (2, 2, 0), (4, 0, 3), (5, 1, 1), (4, 2, 0), (0, 2, 1), (3, 2, 0),
    (2, 1, 2), (0, 3, 0), (4, 1, 2), (2, 2, 1), (5, 2, 0), (4, 2, 1), (4, 3, 0), (2, 3, 0),
)
GATHER = (
    (((0,), (1,), (2,), (3,)), 7),
    (((0,), (2,), (1,), (3,)), 8),
    (((1,), (2,), (0,), (3,)), 6),
    (((2,), (0, 1), (3,)), 6),
)
GATHER_STEPS = (
    (0, 1, 4), (0, 0, 4), (1, 2, 4), (1, 0, 4), (0, 2, 4), (0, 3, 4), (2, 0, 4), (2, 2, 4),
    (1, 1, 4), (3, 1, 3), (1, 3, 4), (2, 1, 4), (2, 3, 4), (0, 1, 3), (3, 0, 3), (0, 0, 3),
    (3, 2, 3), (0, 2, 3), (1, 2, 3), (1, 0, 3), (2, 0, 3), (2, 2, 3), (1, 1, 3), (2, 1, 3),
    (3, 1, 2), (0, 1, 2), (3, 0, 2), (0, 0, 2), (1, 0, 2), (1, 1, 2), (2, 0, 2), (2, 1, 2),
    (0, 0, 1), (3, 0, 1), (1, 0, 1), (2, 0, 1),
)
SHARE_AT, STATES_AT = (4, (0, 6, 9, 12))


def flip(index, mask):
    bit = 1
    while bit <= mask:
        if mask & bit:
            index = index + bit * (1 - 2 * ((index // bit) % 2))
        bit *= 2
    return index


def bits_of(count):
    return count.bit_length() - 1


def split(tiles, weights):
    edges = [tiles * sum(weights[:i]) // sum(weights) for i in range(len(weights) + 1)]
    return [(low * TILE, (high - low) * TILE) for low, high in zip(edges, edges[1:])]


class Route:
    def __init__(self, stages, links):
        self.stages, self.links = stages, links
        self.radix = [1 << len(stage) for stage in stages]
        self.count = []
        below = 1
        for radix in reversed(self.radix):
            self.count.insert(0, below)
            below *= radix
        self.units = below
        self.base = [below - radix * count for radix, count in zip(self.radix, self.count)]
        self.last = len(stages) - 1

    def digit(self, unit, s):
        return unit // self.count[s] % self.radix[s]

    def mask(self, unit):
        a = b = 0
        for s, stage in enumerate(self.stages):
            digit = self.digit(unit, s)
            for i, link in enumerate(stage):
                if digit >> (len(stage) - 1 - i) & 1:
                    a, b = a ^ self.links[link][0], b ^ self.links[link][1]
        return a, b

    def stage_of(self, unit):
        return next((s for s in range(len(self.stages)) if self.digit(unit, s)), len(self.stages))

    def pieces(self, s):
        return list(zip(self.count[s + 1:], self.count[s:])) + [(0, 1)]

    def groups(self, t):
        found = {}
        for d in range(1, self.radix[t]):
            for unit in range(self.count[t]):
                found.setdefault(self.stage_of(unit), []).append((unit, d))
        return found


def numbered(routes, part):
    keys = [(k, s, p) for k, route in enumerate(routes) for s in range(len(route.stages)) for p in part(route, s)]
    return {key: i for i, key in enumerate(keys)}


def numbered_pieces(routes):
    return numbered(routes, lambda route, s: range(len(route.pieces(s))))


def numbered_groups(routes):
    return numbered(routes, Route.groups)


def kernel(n_grp, n_shard, links, reduction, gather, *refs):
    refs = list(refs)
    (routes, flows), (g_routes, g_flows) = reduction, gather
    n_flows, n_gather, n_links = len(flows), len(g_flows), len(links)

    def take(count):
        taken = refs[:count]
        del refs[:count]
        return taken

    count_ref, grads, master, one, two, state = take(6)
    gathered = take(n_gather)
    acc, got, sbuf, rbuf, sscale, rscale = (take(n_flows) for _ in range(6))
    wown = take(n_gather)
    (full, nown, nall, olds, news, meter, steps_ref,
     sems, csend, send, gsend, grecv, nsend, nrecv,
     isem, osem, wsend, lout, xsend, xrecv, tsem) = refs
    pieces, groups = numbered_pieces(routes), numbered_groups(g_routes)
    g, s_me = lax.axis_index("grp"), lax.axis_index("shard")
    rows, cols = master.shape
    core = g % 2

    grp_of = [flip(g, m) for m in range(n_grp)]
    shard_of = [flip(s_me, m) for m in range(n_shard)]
    lane_of = [pl.multiple_of(grp * LANES, LANES) for grp in grp_of]
    dims = list(range(bits_of(n_grp) - 2, -1, -1)) + list(range(n_links - 1, bits_of(n_grp) - 2, -1))
    bit = [g // links[l][0] % 2 if links[l][0] else s_me // links[l][1] % 2 for l in range(n_links)]

    def at(mask):
        return (grp_of[mask[0]], shard_of[mask[1]])

    def place(mask):
        return tuple(
            1 - bit[l] if (mask[0] & links[l][0]) or (mask[1] & links[l][1]) else bit[l] for l in dims)

    def columns(ref, gm):
        return ref.at[:, pl.ds(lane_of[gm], LANES)]

    mate = at((1, 0))
    barrier = pltpu.get_barrier_semaphore()
    peers = sorted({route.mask(d * route.count[s])
                    for route in routes + g_routes for s in range(len(route.stages)) for d in range(1, route.radix[s])})
    pltpu.make_async_copy(count_ref, steps_ref, tsem).start()
    near = [mate] + [at(m) for m in peers]
    for peer in near:
        pl.semaphore_signal(barrier, inc=1, device_id=peer, device_id_type=MESH)

    n_outer = grads.ndim - 2

    def parts(k, part, parity):
        offset, length = flows[k]
        link = routes[k].stages[0][0]
        where = tuple((bit[l] if part == 0 else 1 - bit[l]) if l == link else slice(None) for l in dims)
        head, outer = where[:len(dims) - n_outer], where[len(dims) - n_outer:]
        if any(isinstance(h, slice) for h in head):
            heads = [tuple(y >> i & 1 for i in range(len(head) - 1, -1, -1)) for y in range(1 << len(head))]
        else:
            heads = [head]
        for h in heads:
            grp = sum(b << (len(h) - 1 - i) for i, b in enumerate(h))
            lanes = pl.ds(pl.multiple_of((2 * grp + parity) * LANES, LANES), LANES)
            yield grads.at[outer + (pl.ds(offset, length), lanes)], h + outer

    def cube_part(ref, k, part):
        link = routes[k].stages[0][0]
        return ref.at[tuple((bit[l] if part == 0 else 1 - bit[l]) if l == link else slice(None) for l in dims)]

    def fetch(k, part):
        for source, where in parts(k, part, core):
            pltpu.make_async_copy(source, acc[k].at[where], sems.at[2 * k + part]).start()

    def cross(k, part):
        for source, where in parts(k, part, 1 - core):
            pltpu.make_async_remote_copy(
                src_ref=source, dst_ref=got[k].at[where],
                send_sem=csend, recv_sem=sems.at[2 * (n_flows + k) + part],
                device_id=mate, device_id_type=MESH).start()

    def crossed(k, part):
        ref = cube_part(got[k], k, part)
        return pltpu.make_async_remote_copy(
            src_ref=ref, dst_ref=ref, send_sem=csend, recv_sem=sems.at[2 * (n_flows + k) + part],
            device_id=mate, device_id_type=MESH)

    def loaded(k, part):
        ref = cube_part(acc[k], k, part)
        pltpu.make_async_copy(ref, ref, sems.at[2 * k + part]).wait()

    for k in range(n_flows):
        fetch(k, 1)
    pl.semaphore_wait(barrier, len(near))
    for k in range(n_flows):
        cross(k, 1)
    for k in range(n_flows):
        fetch(k, 0)
        cross(k, 0)

    grp_order = [0]
    for b in range(1, bits_of(n_grp)):
        grp_order = grp_order + [m ^ (1 << b) for m in grp_order]
    grp_order = grp_order + [m ^ 1 for m in grp_order]

    def whole(ref, send, recv):
        return pltpu.make_async_remote_copy(
            src_ref=ref, dst_ref=ref, send_sem=send, recv_sem=recv, device_id=mate, device_id_type=MESH)

    def message(k, s, d, p):
        route = routes[k]
        low, high = route.pieces(s)[p]
        start = route.base[s] + (d - 1) * route.count[s] + low
        span = pl.ds(start, high - low)
        to = at(route.mask(d * route.count[s]))
        return [
            pltpu.make_async_remote_copy(
                src_ref=sscale[k].at[span], dst_ref=rscale[k].at[span],
                send_sem=send, recv_sem=sems.at[4 * n_flows + pieces[k, s, p]], device_id=to, device_id_type=MESH),
            pltpu.make_async_remote_copy(
                src_ref=sbuf[k].at[span], dst_ref=rbuf[k].at[span],
                send_sem=send, recv_sem=sems.at[4 * n_flows + pieces[k, s, p]], device_id=to, device_id_type=MESH),
        ]

    def rows_of(units, length):
        return units * length // 2

    def metered(n, send_sem, recv_sem):
        return whole(meter.at[pl.ds(0, n)], send_sem, recv_sem)

    def await_piece(k, s, p):
        low, high = routes[k].pieces(s)[p]
        units = (routes[k].radix[s] - 1) * (high - low)
        metered(rows_of(units, flows[k][1]) + units, send, sems.at[4 * n_flows + pieces[k, s, p]]).wait_recv()

    def arrived(k, s, unit):
        route = routes[k]
        total = None
        for d in range(1, route.radix[s]):
            i = route.base[s] + (d - 1) * route.count[s] + unit
            value = rbuf[k][i].astype(jnp.int32).astype(jnp.float32) * rscale[k][i]
            total = value if total is None else total + value
        return total

    awaited = set()

    def once(key, *waits):
        if key not in awaited:
            awaited.add(key)
            for wait in waits:
                wait()

    def ready(k, s):
        part = int(s == 0)
        once((k, part), lambda: loaded(k, part), lambda: crossed(k, part).wait_recv())
        for earlier in range(s):
            once((k, s, earlier), lambda: await_piece(k, earlier, s - earlier - 1))

    def summed(k, s, unit):
        where = place(routes[k].mask(unit))
        value = acc[k][where] + got[k][where]
        for earlier in range(s):
            value = value + arrived(k, earlier, unit)
        return value

    def ship(k, s, p):
        route, length = routes[k], flows[k][1]
        ready(k, s)
        count = route.count[s]
        low, high = route.pieces(s)[p]
        for d in range(1, route.radix[s]):
            for r in range(low, high):
                value = summed(k, s, d * count + r)
                most = jnp.max(jnp.abs(value).reshape(length // 8, 8, LANES), axis=0)
                top = jnp.maximum(jnp.max(most, axis=0, keepdims=True), 1e-30)
                i = route.base[s] + (d - 1) * count + r
                sscale[k][i] = top * (1.0 / LEVELS)
                sbuf[k][i] = jnp.round(value * (LEVELS / top)).astype(jnp.int32).astype(jnp.int16)
            for copy in message(k, s, d, p):
                copy.start()

    def load_state():
        for n, source in enumerate((master, one, two)):
            for i, gm in enumerate(grp_order):
                pltpu.make_async_copy(columns(source, gm), olds.at[n, i], isem).start()

    def finish(k):
        offset, length = flows[k]
        n_stages = len(routes[k].stages)
        ready(k, n_stages)
        value = summed(k, n_stages, 0)
        full[0, offset:offset + length] = value
        return jnp.sum((value * value).reshape(length // 8, 8, LANES), axis=0)

    for index, step in enumerate(REDUCE_STEPS):
        if index == 2 * n_flows:
            load_state()
        ship(*step)
    squares = jnp.zeros((8, LANES), jnp.float32)
    for k in range(n_flows):
        squares = squares + finish(k)
    nown[...] = jnp.sum(squares, axis=0, keepdims=True)
    me = g * n_shard + s_me
    everyone = n_grp * n_shard

    def tell(gm, sm):
        return pltpu.make_async_remote_copy(
            src_ref=nown, dst_ref=nall.at[me], send_sem=nsend, recv_sem=nrecv,
            device_id=at((gm, sm)), device_id_type=MESH)

    for gm in reversed(range(n_grp)):
        for sm in reversed(range(n_shard)):
            if gm or sm:
                tell(gm, sm).start()
    nall[me] = nown[...]

    def share(n, mask, index):
        return pltpu.make_async_remote_copy(
            src_ref=full.at[pl.ds(0, n)], dst_ref=full.at[pl.ds(n, n)],
            send_sem=gsend.at[index], recv_sem=grecv.at[index], device_id=at((mask, 0)), device_id_type=MESH)

    shares = []
    for index in range(bits_of(n_grp)):
        mask = 1 if index == bits_of(n_grp) - 1 else 2 << index
        shares.append(share(1 << index, mask, index))
    for index in range(len(shares) - 1):
        shares[index].start()
        if index < len(shares) - 2:
            shares[index].wait_recv()

    pltpu.make_async_copy(olds, olds, isem).wait()
    pltpu.make_async_copy(count_ref, steps_ref, tsem).wait()
    t = jnp.full((8, LANES), steps_ref[0], jnp.int32).astype(jnp.float32)
    first_fix = (1.0 - jnp.power(jnp.full((8, LANES), 0.9, jnp.float32), t))[0:1]
    second_fix = (1.0 - jnp.power(jnp.full((8, LANES), 0.999, jnp.float32), t))[0:1]
    others = nall.at[pl.ds(0, everyone - 1)]
    whole(others, nsend, nrecv).wait()
    norm = jnp.sqrt(jnp.sum(jnp.sum(nall[...], axis=0), axis=1, keepdims=True))
    clip = jnp.minimum(1.0, 1.0 / (norm + 1e-6))

    def update(i, k):
        offset, length = g_flows[k]
        tiles = length // TILE
        group = max(d for d in range(1, 6) if tiles % d == 0) * TILE

        def body(r, carry):
            span = pl.ds(pl.multiple_of(offset + r * group, TILE), group)
            gradient = clip * full[i, span]
            m_one = 0.9 * olds[1, i, span] + 0.1 * gradient
            m_two = 0.999 * olds[2, i, span] + 0.001 * gradient * gradient
            step = m_one / first_fix / (jnp.sqrt(m_two / second_fix) + 1e-8)
            old = olds[0, i, span]
            fresh = old - 0.01 * (step + 0.01 * old)
            news[0, i, span] = fresh
            news[1, i, span] = m_one
            news[2, i, span] = m_two
            if i == 0:
                wown[k][pl.ds(pl.multiple_of(r * group, TILE), group)] = fresh.astype(jnp.bfloat16)
            return carry

        lax.fori_loop(0, length // group, body, 0)

    def slot(k, unit):
        return gathered[k].at[(core,) + place(g_routes[k].mask(unit))]

    def push(k, unit, s, d):
        route = g_routes[k]
        return pltpu.make_async_remote_copy(
            src_ref=slot(k, unit) if unit else wown[k], dst_ref=slot(k, unit),
            send_sem=wsend, recv_sem=sems.at[groups[k, s, route.stage_of(unit)]],
            device_id=at(route.mask(d * route.count[s])), device_id_type=MESH)

    def forward(k, unit):
        route = g_routes[k]
        for s in range(route.stage_of(unit) - 1, -1, -1):
            for d in range(1, route.radix[s]):
                push(k, unit, s, d).start()
        pltpu.make_async_remote_copy(
            src_ref=slot(k, unit) if unit else wown[k], dst_ref=slot(k, unit),
            send_sem=xsend, recv_sem=xrecv, device_id=mate, device_id_type=MESH).start()
        if unit == 0:
            pltpu.make_async_copy(wown[k], slot(k, 0), lout).start()

    def arrive(k, t, origin):
        route = g_routes[k]
        members = route.groups(t)[origin]
        metered(rows_of(len(members), g_flows[k][1]), wsend, sems.at[groups[k, t, origin]]).wait_recv()
        for unit, d in members:
            forward(k, unit + d * route.count[t])


    def share_on():
        if len(shares) > 1:
            shares[-2].wait_recv()
        shares[-1].start()

    def states(i):
        if i == len(grp_order) // 2:
            shares[-1].wait_recv()
        if i:
            for k in range(n_gather):
                update(i, k)
        for n in range(3):
            pltpu.make_async_copy(news.at[n, i], columns(state.at[n], grp_order[i]), osem).start()

    for k in range(n_gather):
        update(0, k)
        forward(k, 0)
    for index in range(len(GATHER_STEPS) + 1):
        if index == SHARE_AT:
            share_on()
        for i, when in enumerate(STATES_AT):
            if index == when:
                states(i)
        if index < len(GATHER_STEPS):
            arrive(*GATHER_STEPS[index])

    n_units = routes[0].units
    metered(n_units * rows, csend, nrecv).wait_send()
    metered(rows_of(n_units - 1, rows) + n_flows * (n_units - 1), send, nrecv).wait_send()
    metered(rows_of(n_units - 1, rows), wsend, nrecv).wait_send()
    for copy in shares:
        copy.wait_send()
    own = meter.at[pl.ds(0, rows // 2)]
    pltpu.make_async_copy(own, own, lout).wait()
    pltpu.make_async_copy(news, news, osem).wait()
    metered(rows_of(n_units, rows), xsend, xrecv).wait()


def place_out(flows, n_outer, *refs):
    n_flows = len(flows)
    state, gathered = refs[0], refs[1:1 + n_flows]
    outs, weights, outs_sem, weights_sem = refs[1 + n_flows:4 + n_flows], *refs[4 + n_flows:]
    for k, (offset, length) in enumerate(flows):
        n_head = gathered[k].ndim - 2 - n_outer
        for i in range(1 << n_head):
            head = tuple(i >> b & 1 for b in range(n_head))
            grp = sum(h << b for b, h in enumerate(head))
            where = (slice(None),) * n_outer + (pl.ds(offset, length), pl.ds(grp * LANES, LANES))
            head = head[:1] + head[:0:-1]
            pltpu.make_async_copy(gathered[k].at[head], weights.at[where], weights_sem).start()
    for n in range(3):
        pltpu.make_async_copy(state.at[n], outs[n], outs_sem).start()
    pltpu.make_async_copy(state, state, outs_sem).wait()
    pltpu.make_async_copy(weights, weights, weights_sem).wait()


def fused(mesh, grads, master, moment_one, moment_two, step_count):
    n_grp, n_shard = mesh.shape["grp"], mesh.shape["shard"]
    rows, cols = master.shape
    links = [(2 << i, 0) for i in range(bits_of(n_grp) - 1)] + [(0, 1 << i) for i in range(bits_of(n_shard))]
    n_links, n_units = len(links), 1 << len(links)
    reduction, gather = (
        ([Route(stages, links) for stages, _ in entries], split(rows // TILE, [weight for _, weight in entries]))
        for entries in (REDUCE, GATHER))
    flows, g_flows = reduction[1], gather[1]
    n_flows, n_gather, n_outer = len(flows), len(g_flows), bits_of(n_shard)
    vmem, dma = pltpu.VMEM, pltpu.SemaphoreType.DMA
    any_space, hbm_space = pl.BlockSpec(memory_space=pl.ANY), pl.BlockSpec(memory_space=pltpu.HBM)
    n_share = bits_of(n_grp)
    n_pieces, n_groups = len(numbered_pieces(reduction[0])), len(numbered_groups(gather[0]))
    cube = (2,) * n_links
    scratch = []
    for _ in range(2):
        scratch += [vmem(cube + (length, LANES), jnp.float32) for _, length in flows]
    for _ in range(2):
        scratch += [vmem((n_units - 1, length, LANES), jnp.int16) for _, length in flows]
    for _ in range(2):
        scratch += [vmem((n_units - 1, 1, LANES), jnp.float32) for _ in flows]
    scratch += [vmem((length, LANES), jnp.bfloat16) for _, length in g_flows]
    scratch += [
        vmem((n_grp, rows, LANES), jnp.float32),
        vmem((1, LANES), jnp.float32),
        vmem((n_grp * n_shard, 1, LANES), jnp.float32),
        vmem((3, n_grp, rows, LANES), jnp.float32),
        vmem((3, n_grp, rows, LANES), jnp.float32),
        vmem((n_units * rows, 1, LANES), jnp.float32),
        pltpu.SMEM((1,), jnp.int32),
        dma((max(4 * n_flows + n_pieces, n_groups),)), dma, dma, dma((n_share,)), dma((n_share,)), dma, dma,
        dma, dma, dma, dma, dma, dma, dma,
    ]
    cut = (2,) * n_outer + (rows, cols)
    state, *gathered = pl.pallas_call(
        functools.partial(kernel, n_grp, n_shard, links, reduction, gather),
        out_shape=[jax.ShapeDtypeStruct((3, rows, cols), jnp.float32)] + [
            jax.ShapeDtypeStruct((2,) + cube + (length, LANES), jnp.bfloat16) for _, length in g_flows],
        in_specs=[any_space] + [hbm_space] * 4,
        out_specs=[any_space] * (1 + n_gather),
        scratch_shapes=scratch,
        compiler_params=pltpu.CompilerParams(collective_id=0, has_side_effects=True, vmem_limit_bytes=VMEM_LIMIT),
    )(step_count, *(pltpu.with_memory_space_constraint(x, pltpu.HBM)
                    for x in (grads[0, 0].reshape(cut), master, moment_one, moment_two)))
    *outs, weights = pl.pallas_call(
        functools.partial(place_out, g_flows, n_outer),
        out_shape=[jax.ShapeDtypeStruct((rows, cols), jnp.float32)] * 3 + [jax.ShapeDtypeStruct(cut, jnp.bfloat16)],
        in_specs=[any_space] * (1 + n_gather),
        out_specs=[hbm_space] * 4,
        scratch_shapes=[dma, dma],
        compiler_params=pltpu.CompilerParams(vmem_limit_bytes=1 << 20),
    )(state, *gathered)
    return (*outs, weights.reshape(rows * n_shard, cols))


def plain(grads, master, moment_one, moment_two, step_count):
    local = grads[0, 0]
    count = master.shape[0]
    total = lax.psum(local, ("grp", "shard"))
    squares = jnp.sum(total * total)
    start = lax.axis_index("shard") * count
    gradient = lax.dynamic_slice_in_dim(total, start, count, 0)
    norm = jnp.sqrt(squares)
    clip = jnp.minimum(jnp.float32(1.0), 1.0 / (norm + 1e-06))
    gradient = clip * gradient
    new_one = 0.9 * moment_one + 0.1 * gradient
    new_two = 0.999 * moment_two + 0.001 * gradient * gradient
    steps = step_count[0].astype(jnp.float32)
    first_fix = 1.0 - jnp.power(jnp.float32(0.9), steps)
    second_fix = 1.0 - jnp.power(jnp.float32(0.999), steps)
    update = new_one / first_fix / (jnp.sqrt(new_two / second_fix) + 1e-08)
    new_master = master - 0.01 * (update + 0.01 * master)
    weights = lax.all_gather(new_master.astype(jnp.bfloat16), "shard", axis=0, tiled=True)
    return (new_master, new_one, new_two, weights)


def solution(mesh):
    n_grp, n_shard = mesh.shape["grp"], mesh.shape["shard"]

    def shards(grads, master, moment_one, moment_two, step_count):
        rows, cols = master.shape
        powers = all(n & (n - 1) == 0 for n in (n_grp, n_shard))
        links = bits_of(n_grp) - 1 + bits_of(n_shard)
        matched = {link for stages, _ in REDUCE for stage in stages for link in stage} == set(range(links))
        if powers and n_grp > 2 and matched and cols == LANES * n_grp and rows % TILE == 0:
            return fused(mesh, grads, master, moment_one, moment_two, step_count)
        return plain(grads, master, moment_one, moment_two, step_count)

    return jax.shard_map(
        shards,
        mesh=mesh,
        in_specs=(
            P("grp", "shard", None, None),
            P("shard", None),
            P("shard", None),
            P("shard", None),
            P(),
        ),
        out_specs=(P("shard", None), P("shard", None), P("shard", None), P()),
        check_vma=False,
    )
```

```python
import functools
import jax
import jax.numpy as jnp
from jax import lax
from jax.experimental import pallas as pl
from jax.experimental.pallas import tpu as pltpu
from jax.sharding import PartitionSpec as P

MESH = pl.DeviceIdType.MESH
LANES = 128
TILE = 16
LEVELS = 32767.0
VMEM_LIMIT = 44 << 20

REDUCE = (
    (((2,), (0,), (1,), (3,)), 3),
    (((0,), (1,), (2, 3)), 4),
    (((0,), (1,), (3,), (2,)), 5),
    (((1,), (3,), (2, 0)), 5),
    (((2,), (0,), (1,), (3,)), 8),
    (((1,), (0,), (2, 3)), 2),
)
REDUCE_STEPS = (
    (0, 0, 0), (1, 0, 0), (2, 0, 0), (0, 0, 1), (3, 0, 0), (1, 0, 1), (4, 0, 0), (2, 0, 1),
    (5, 0, 0), (3, 0, 1), (0, 0, 2), (0, 1, 0), (4, 0, 1), (1, 0, 2), (1, 1, 0), (5, 0, 1),
    (2, 0, 2), (3, 1, 0), (3, 0, 2), (2, 1, 0), (0, 0, 3), (4, 0, 2), (0, 1, 1), (4, 1, 0),
    (5, 0, 2), (1, 1, 1), (5, 1, 0), (2, 0, 3), (3, 1, 1), (0, 2, 0), (2, 1, 1), (1, 2, 0),
    (4, 0, 3), (0, 1, 2), (4, 1, 1), (2, 2, 0), (5, 1, 1), (4, 2, 0), (0, 2, 1), (3, 2, 0),
    (2, 1, 2), (0, 3, 0), (4, 1, 2), (2, 2, 1), (5, 2, 0), (4, 2, 1), (4, 3, 0), (2, 3, 0),
)
GATHER = (
    (((0,), (1,), (2,), (3,)), 7),
    (((0,), (2,), (1,), (3,)), 8),
    (((1,), (2,), (0,), (3,)), 6),
    (((2,), (0, 1), (3,)), 6),
)
GATHER_STEPS = (
    (0, 1, 4), (0, 0, 4), (1, 2, 4), (1, 0, 4), (0, 2, 4), (0, 3, 4), (2, 0, 4), (2, 2, 4),
    (1, 1, 4), (3, 1, 3), (1, 3, 4), (2, 1, 4), (2, 3, 4), (0, 1, 3), (3, 0, 3), (0, 0, 3),
    (3, 2, 3), (0, 2, 3), (1, 2, 3), (1, 0, 3), (2, 0, 3), (2, 2, 3), (1, 1, 3), (2, 1, 3),
    (3, 1, 2), (0, 1, 2), (3, 0, 2), (0, 0, 2), (1, 0, 2), (1, 1, 2), (2, 0, 2), (2, 1, 2),
    (0, 0, 1), (3, 0, 1), (1, 0, 1), (2, 0, 1),
)
SHARE_AT, STATES_AT = (4, (0, 6, 9, 12))


def flip(index, mask):
    bit = 1
    while bit <= mask:
        if mask & bit:
            index = index + bit * (1 - 2 * ((index // bit) % 2))
        bit *= 2
    return index


def bits_of(count):
    return count.bit_length() - 1


def split(tiles, weights):
    edges = [tiles * sum(weights[:i]) // sum(weights) for i in range(len(weights) + 1)]
    return [(low * TILE, (high - low) * TILE) for low, high in zip(edges, edges[1:])]


class Route:
    def __init__(self, stages, links):
        self.stages, self.links = stages, links
        self.radix = [1 << len(stage) for stage in stages]
        self.count = []
        below = 1
        for radix in reversed(self.radix):
            self.count.insert(0, below)
            below *= radix
        self.units = below
        self.base = [below - radix * count for radix, count in zip(self.radix, self.count)]
        self.last = len(stages) - 1

    def digit(self, unit, s):
        return unit // self.count[s] % self.radix[s]

    def mask(self, unit):
        a = b = 0
        for s, stage in enumerate(self.stages):
            digit = self.digit(unit, s)
            for i, link in enumerate(stage):
                if digit >> (len(stage) - 1 - i) & 1:
                    a, b = a ^ self.links[link][0], b ^ self.links[link][1]
        return a, b

    def stage_of(self, unit):
        return next((s for s in range(len(self.stages)) if self.digit(unit, s)), len(self.stages))

    def pieces(self, s):
        return list(zip(self.count[s + 1:], self.count[s:])) + [(0, 1)]

    def groups(self, t):
        found = {}
        for d in range(1, self.radix[t]):
            for unit in range(self.count[t]):
                found.setdefault(self.stage_of(unit), []).append((unit, d))
        return found


def numbered(routes, part):
    keys = [(k, s, p) for k, route in enumerate(routes) for s in range(len(route.stages)) for p in part(route, s)]
    return {key: i for i, key in enumerate(keys)}


def numbered_pieces(routes):
    return numbered(routes, lambda route, s: range(len(route.pieces(s))))


def numbered_groups(routes):
    return numbered(routes, Route.groups)


def kernel(n_grp, n_shard, links, reduction, gather, *refs):
    refs = list(refs)
    (routes, flows), (g_routes, g_flows) = reduction, gather
    n_flows, n_gather, n_links = len(flows), len(g_flows), len(links)

    def take(count):
        taken = refs[:count]
        del refs[:count]
        return taken

    count_ref, grads, master, one, two, state = take(6)
    gathered = take(n_gather)
    acc, got, sbuf, rbuf, sscale, rscale = (take(n_flows) for _ in range(6))
    wown = take(n_gather)
    (full, nown, nall, olds, news, meter, steps_ref,
     sems, csend, send, gsend, grecv, nsend, nrecv,
     isem, osem, wsend, lout, xsend, xrecv, tsem) = refs
    pieces, groups = numbered_pieces(routes), numbered_groups(g_routes)
    g, s_me = lax.axis_index("grp"), lax.axis_index("shard")
    rows, cols = master.shape
    core = g % 2

    grp_of = [flip(g, m) for m in range(n_grp)]
    shard_of = [flip(s_me, m) for m in range(n_shard)]
    lane_of = [pl.multiple_of(grp * LANES, LANES) for grp in grp_of]
    dims = list(range(bits_of(n_grp) - 2, -1, -1)) + list(range(n_links - 1, bits_of(n_grp) - 2, -1))
    bit = [g // links[l][0] % 2 if links[l][0] else s_me // links[l][1] % 2 for l in range(n_links)]

    def at(mask):
        return (grp_of[mask[0]], shard_of[mask[1]])

    def place(mask):
        return tuple(
            1 - bit[l] if (mask[0] & links[l][0]) or (mask[1] & links[l][1]) else bit[l] for l in dims)

    def columns(ref, gm):
        return ref.at[:, pl.ds(lane_of[gm], LANES)]

    mate = at((1, 0))
    barrier = pltpu.get_barrier_semaphore()
    peers = sorted({route.mask(d * route.count[s])
                    for route in routes + g_routes for s in range(len(route.stages)) for d in range(1, route.radix[s])})
    pltpu.make_async_copy(count_ref, steps_ref, tsem).start()
    near = [mate] + [at(m) for m in peers]
    for peer in near:
        pl.semaphore_signal(barrier, inc=1, device_id=peer, device_id_type=MESH)

    n_outer = grads.ndim - 2

    def parts(k, part, parity):
        offset, length = flows[k]
        link = routes[k].stages[0][0]
        where = tuple((bit[l] if part == 0 else 1 - bit[l]) if l == link else slice(None) for l in dims)
        head, outer = where[:len(dims) - n_outer], where[len(dims) - n_outer:]
        if any(isinstance(h, slice) for h in head):
            heads = [tuple(y >> i & 1 for i in range(len(head) - 1, -1, -1)) for y in range(1 << len(head))]
        else:
            heads = [head]
        for h in heads:
            grp = sum(b << (len(h) - 1 - i) for i, b in enumerate(h))
            lanes = pl.ds(pl.multiple_of((2 * grp + parity) * LANES, LANES), LANES)
            yield grads.at[outer + (pl.ds(offset, length), lanes)], h + outer

    def fetch(k, part):
        for source, where in parts(k, part, core):
            pltpu.make_async_copy(source, acc[k].at[where], sems.at[2 * k + part]).start()

    def cross(k, part):
        for source, where in parts(k, part, 1 - core):
            pltpu.make_async_remote_copy(
                src_ref=source, dst_ref=got[k].at[where],
                send_sem=csend, recv_sem=sems.at[2 * k + part],
                device_id=mate, device_id_type=MESH).start()

    def both(k, part):
        n = routes[k].units * flows[k][1]
        pltpu.make_async_copy(meter.at[pl.ds(0, n)], meter.at[pl.ds(0, n)], sems.at[2 * k + part]).wait()

    for k in range(n_flows):
        fetch(k, 1)
    pl.semaphore_wait(barrier, len(near))
    for k in range(n_flows):
        cross(k, 1)
    for k in range(n_flows):
        fetch(k, 0)
        cross(k, 0)

    grp_order = [0]
    for b in range(1, bits_of(n_grp)):
        grp_order = grp_order + [m ^ (1 << b) for m in grp_order]
    grp_order = grp_order + [m ^ 1 for m in grp_order]

    def whole(ref, send, recv):
        return pltpu.make_async_remote_copy(
            src_ref=ref, dst_ref=ref, send_sem=send, recv_sem=recv, device_id=mate, device_id_type=MESH)

    def message(k, s, d, p):
        route = routes[k]
        low, high = route.pieces(s)[p]
        start = route.base[s] + (d - 1) * route.count[s] + low
        span = pl.ds(start, high - low)
        to = at(route.mask(d * route.count[s]))
        return [
            pltpu.make_async_remote_copy(
                src_ref=sscale[k].at[span], dst_ref=rscale[k].at[span],
                send_sem=send, recv_sem=sems.at[2 * n_flows + pieces[k, s, p]], device_id=to, device_id_type=MESH),
            pltpu.make_async_remote_copy(
                src_ref=sbuf[k].at[span], dst_ref=rbuf[k].at[span],
                send_sem=send, recv_sem=sems.at[2 * n_flows + pieces[k, s, p]], device_id=to, device_id_type=MESH),
        ]

    def rows_of(units, length):
        return units * length // 2

    def metered(n, send_sem, recv_sem):
        return whole(meter.at[pl.ds(0, n)], send_sem, recv_sem)

    def await_piece(k, s, p):
        low, high = routes[k].pieces(s)[p]
        units = (routes[k].radix[s] - 1) * (high - low)
        metered(rows_of(units, flows[k][1]) + units, send, sems.at[2 * n_flows + pieces[k, s, p]]).wait_recv()

    def arrived(k, s, unit):
        route = routes[k]
        total = None
        for d in range(1, route.radix[s]):
            i = route.base[s] + (d - 1) * route.count[s] + unit
            value = rbuf[k][i].astype(jnp.int32).astype(jnp.float32) * rscale[k][i]
            total = value if total is None else total + value
        return total

    awaited = set()

    def once(key, *waits):
        if key not in awaited:
            awaited.add(key)
            for wait in waits:
                wait()

    def ready(k, s):
        part = int(s == 0)
        once((k, part), lambda: both(k, part))
        for earlier in range(s):
            once((k, s, earlier), lambda: await_piece(k, earlier, s - earlier - 1))

    def summed(k, s, unit):
        where = place(routes[k].mask(unit))
        value = acc[k][where] + got[k][where]
        for earlier in range(s):
            value = value + arrived(k, earlier, unit)
        return value

    def ship(k, s, p):
        route, length = routes[k], flows[k][1]
        ready(k, s)
        count = route.count[s]
        low, high = route.pieces(s)[p]
        for d in range(1, route.radix[s]):
            for r in range(low, high):
                value = summed(k, s, d * count + r)
                most = jnp.max(jnp.abs(value).reshape(length // 8, 8, LANES), axis=0)
                top = jnp.maximum(jnp.max(most, axis=0, keepdims=True), 1e-30)
                i = route.base[s] + (d - 1) * count + r
                sscale[k][i] = top * (1.0 / LEVELS)
                sbuf[k][i] = jnp.round(value * (LEVELS / top)).astype(jnp.int32).astype(jnp.int16)
            for copy in message(k, s, d, p):
                copy.start()

    def load_state():
        for n, source in enumerate((master, one, two)):
            for i, gm in enumerate(grp_order):
                pltpu.make_async_copy(columns(source, gm), olds.at[n, i], isem).start()

    def finish(k):
        offset, length = flows[k]
        n_stages = len(routes[k].stages)
        ready(k, n_stages)
        value = summed(k, n_stages, 0)
        full[0, offset:offset + length] = value
        return jnp.sum((value * value).reshape(length // 8, 8, LANES), axis=0)

    for index, step in enumerate(REDUCE_STEPS):
        if index == 2 * n_flows:
            load_state()
        ship(*step)
    squares = jnp.zeros((8, LANES), jnp.float32)
    for k in range(n_flows):
        squares = squares + finish(k)
    nown[...] = jnp.sum(squares, axis=0, keepdims=True)
    me = g * n_shard + s_me
    everyone = n_grp * n_shard

    def tell(gm, sm):
        return pltpu.make_async_remote_copy(
            src_ref=nown, dst_ref=nall.at[me], send_sem=nsend, recv_sem=nrecv,
            device_id=at((gm, sm)), device_id_type=MESH)

    for gm in reversed(range(n_grp)):
        for sm in reversed(range(n_shard)):
            if gm or sm:
                tell(gm, sm).start()
    nall[me] = nown[...]

    def share(n, mask, index):
        return pltpu.make_async_remote_copy(
            src_ref=full.at[pl.ds(0, n)], dst_ref=full.at[pl.ds(n, n)],
            send_sem=gsend.at[index], recv_sem=grecv.at[index], device_id=at((mask, 0)), device_id_type=MESH)

    shares = []
    for index in range(bits_of(n_grp)):
        mask = 1 if index == bits_of(n_grp) - 1 else 2 << index
        shares.append(share(1 << index, mask, index))
    for index in range(len(shares) - 1):
        shares[index].start()
        if index < len(shares) - 2:
            shares[index].wait_recv()

    pltpu.make_async_copy(olds, olds, isem).wait()
    pltpu.make_async_copy(count_ref, steps_ref, tsem).wait()
    t = jnp.full((8, LANES), steps_ref[0], jnp.int32).astype(jnp.float32)
    first_fix = (1.0 - jnp.power(jnp.full((8, LANES), 0.9, jnp.float32), t))[0:1]
    second_fix = (1.0 - jnp.power(jnp.full((8, LANES), 0.999, jnp.float32), t))[0:1]
    others = nall.at[pl.ds(0, everyone - 1)]
    whole(others, nsend, nrecv).wait()
    norm = jnp.sqrt(jnp.sum(jnp.sum(nall[...], axis=0), axis=1, keepdims=True))
    clip = jnp.minimum(1.0, 1.0 / (norm + 1e-6))

    def update(i, k):
        offset, length = g_flows[k]
        tiles = length // TILE
        group = max(d for d in range(1, 6) if tiles % d == 0) * TILE

        def body(r, carry):
            span = pl.ds(pl.multiple_of(offset + r * group, TILE), group)
            gradient = clip * full[i, span]
            m_one = 0.9 * olds[1, i, span] + 0.1 * gradient
            m_two = 0.999 * olds[2, i, span] + 0.001 * gradient * gradient
            step = m_one / first_fix / (jnp.sqrt(m_two / second_fix) + 1e-8)
            old = olds[0, i, span]
            fresh = old - 0.01 * (step + 0.01 * old)
            news[0, i, span] = fresh
            news[1, i, span] = m_one
            news[2, i, span] = m_two
            if i == 0:
                wown[k][pl.ds(pl.multiple_of(r * group, TILE), group)] = fresh.astype(jnp.bfloat16)
            return carry

        lax.fori_loop(0, length // group, body, 0)

    def slot(k, unit):
        return gathered[k].at[(core,) + place(g_routes[k].mask(unit))]

    def push(k, unit, s, d):
        route = g_routes[k]
        return pltpu.make_async_remote_copy(
            src_ref=slot(k, unit) if unit else wown[k], dst_ref=slot(k, unit),
            send_sem=wsend, recv_sem=sems.at[groups[k, s, route.stage_of(unit)]],
            device_id=at(route.mask(d * route.count[s])), device_id_type=MESH)

    def forward(k, unit):
        route = g_routes[k]
        for s in range(route.stage_of(unit) - 1, -1, -1):
            for d in range(1, route.radix[s]):
                push(k, unit, s, d).start()
        pltpu.make_async_remote_copy(
            src_ref=slot(k, unit) if unit else wown[k], dst_ref=slot(k, unit),
            send_sem=xsend, recv_sem=xrecv, device_id=mate, device_id_type=MESH).start()
        if unit == 0:
            pltpu.make_async_copy(wown[k], slot(k, 0), lout).start()

    def arrive(k, t, origin):
        route = g_routes[k]
        members = route.groups(t)[origin]
        metered(rows_of(len(members), g_flows[k][1]), wsend, sems.at[groups[k, t, origin]]).wait_recv()
        for unit, d in members:
            forward(k, unit + d * route.count[t])


    def share_on():
        if len(shares) > 1:
            shares[-2].wait_recv()
        shares[-1].start()

    def states(i):
        if i == len(grp_order) // 2:
            shares[-1].wait_recv()
        if i:
            for k in range(n_gather):
                update(i, k)
        for n in range(3):
            pltpu.make_async_copy(news.at[n, i], columns(state.at[n], grp_order[i]), osem).start()

    for k in range(n_gather):
        update(0, k)
        forward(k, 0)
    for index in range(len(GATHER_STEPS) + 1):
        if index == SHARE_AT:
            share_on()
        for i, when in enumerate(STATES_AT):
            if index == when:
                states(i)
        if index < len(GATHER_STEPS):
            arrive(*GATHER_STEPS[index])

    n_units = routes[0].units
    metered(n_units * rows, csend, nrecv).wait_send()
    metered(rows_of(n_units - 1, rows) + n_flows * (n_units - 1), send, nrecv).wait_send()
    metered(rows_of(n_units - 1, rows), wsend, nrecv).wait_send()
    for copy in shares:
        copy.wait_send()
    own = meter.at[pl.ds(0, rows // 2)]
    pltpu.make_async_copy(own, own, lout).wait()
    pltpu.make_async_copy(news, news, osem).wait()
    metered(rows_of(n_units, rows), xsend, xrecv).wait()


def place_out(flows, n_outer, *refs):
    n_flows = len(flows)
    state, gathered = refs[0], refs[1:1 + n_flows]
    outs, weights, outs_sem, weights_sem = refs[1 + n_flows:4 + n_flows], *refs[4 + n_flows:]
    for k, (offset, length) in enumerate(flows):
        n_head = gathered[k].ndim - 2 - n_outer
        for i in range(1 << n_head):
            head = tuple(i >> b & 1 for b in range(n_head))
            grp = sum(h << b for b, h in enumerate(head))
            where = (slice(None),) * n_outer + (pl.ds(offset, length), pl.ds(grp * LANES, LANES))
            head = head[:1] + head[:0:-1]
            pltpu.make_async_copy(gathered[k].at[head], weights.at[where], weights_sem).start()
    for n in range(3):
        pltpu.make_async_copy(state.at[n], outs[n], outs_sem).start()
    pltpu.make_async_copy(state, state, outs_sem).wait()
    pltpu.make_async_copy(weights, weights, weights_sem).wait()


def fused(mesh, grads, master, moment_one, moment_two, step_count):
    n_grp, n_shard = mesh.shape["grp"], mesh.shape["shard"]
    rows, cols = master.shape
    links = [(2 << i, 0) for i in range(bits_of(n_grp) - 1)] + [(0, 1 << i) for i in range(bits_of(n_shard))]
    n_links, n_units = len(links), 1 << len(links)
    reduction, gather = (
        ([Route(stages, links) for stages, _ in entries], split(rows // TILE, [weight for _, weight in entries]))
        for entries in (REDUCE, GATHER))
    flows, g_flows = reduction[1], gather[1]
    n_flows, n_gather, n_outer = len(flows), len(g_flows), bits_of(n_shard)
    vmem, dma = pltpu.VMEM, pltpu.SemaphoreType.DMA
    any_space, hbm_space = pl.BlockSpec(memory_space=pl.ANY), pl.BlockSpec(memory_space=pltpu.HBM)
    n_share = bits_of(n_grp)
    n_pieces, n_groups = len(numbered_pieces(reduction[0])), len(numbered_groups(gather[0]))
    cube = (2,) * n_links
    scratch = []
    for _ in range(2):
        scratch += [vmem(cube + (length, LANES), jnp.float32) for _, length in flows]
    for _ in range(2):
        scratch += [vmem((n_units - 1, length, LANES), jnp.int16) for _, length in flows]
    for _ in range(2):
        scratch += [vmem((n_units - 1, 1, LANES), jnp.float32) for _ in flows]
    scratch += [vmem((length, LANES), jnp.bfloat16) for _, length in g_flows]
    scratch += [
        vmem((n_grp, rows, LANES), jnp.float32),
        vmem((1, LANES), jnp.float32),
        vmem((n_grp * n_shard, 1, LANES), jnp.float32),
        vmem((3, n_grp, rows, LANES), jnp.float32),
        vmem((3, n_grp, rows, LANES), jnp.float32),
        vmem((n_units * rows, 1, LANES), jnp.float32),
        pltpu.SMEM((1,), jnp.int32),
        dma((max(2 * n_flows + n_pieces, n_groups),)), dma, dma, dma((n_share,)), dma((n_share,)), dma, dma,
        dma, dma, dma, dma, dma, dma, dma,
    ]
    cut = (2,) * n_outer + (rows, cols)
    state, *gathered = pl.pallas_call(
        functools.partial(kernel, n_grp, n_shard, links, reduction, gather),
        out_shape=[jax.ShapeDtypeStruct((3, rows, cols), jnp.float32)] + [
            jax.ShapeDtypeStruct((2,) + cube + (length, LANES), jnp.bfloat16) for _, length in g_flows],
        in_specs=[any_space] + [hbm_space] * 4,
        out_specs=[any_space] * (1 + n_gather),
        scratch_shapes=scratch,
        compiler_params=pltpu.CompilerParams(collective_id=0, has_side_effects=True, vmem_limit_bytes=VMEM_LIMIT),
    )(step_count, *(pltpu.with_memory_space_constraint(x, pltpu.HBM)
                    for x in (grads[0, 0].reshape(cut), master, moment_one, moment_two)))
    *outs, weights = pl.pallas_call(
        functools.partial(place_out, g_flows, n_outer),
        out_shape=[jax.ShapeDtypeStruct((rows, cols), jnp.float32)] * 3 + [jax.ShapeDtypeStruct(cut, jnp.bfloat16)],
        in_specs=[any_space] * (1 + n_gather),
        out_specs=[hbm_space] * 4,
        scratch_shapes=[dma, dma],
        compiler_params=pltpu.CompilerParams(vmem_limit_bytes=1 << 20),
    )(state, *gathered)
    return (*outs, weights.reshape(rows * n_shard, cols))


def plain(grads, master, moment_one, moment_two, step_count):
    local = grads[0, 0]
    count = master.shape[0]
    total = lax.psum(local, ("grp", "shard"))
    squares = jnp.sum(total * total)
    start = lax.axis_index("shard") * count
    gradient = lax.dynamic_slice_in_dim(total, start, count, 0)
    norm = jnp.sqrt(squares)
    clip = jnp.minimum(jnp.float32(1.0), 1.0 / (norm + 1e-06))
    gradient = clip * gradient
    new_one = 0.9 * moment_one + 0.1 * gradient
    new_two = 0.999 * moment_two + 0.001 * gradient * gradient
    steps = step_count[0].astype(jnp.float32)
    first_fix = 1.0 - jnp.power(jnp.float32(0.9), steps)
    second_fix = 1.0 - jnp.power(jnp.float32(0.999), steps)
    update = new_one / first_fix / (jnp.sqrt(new_two / second_fix) + 1e-08)
    new_master = master - 0.01 * (update + 0.01 * master)
    weights = lax.all_gather(new_master.astype(jnp.bfloat16), "shard", axis=0, tiled=True)
    return (new_master, new_one, new_two, weights)


def solution(mesh):
    n_grp, n_shard = mesh.shape["grp"], mesh.shape["shard"]

    def shards(grads, master, moment_one, moment_two, step_count):
        rows, cols = master.shape
        powers = all(n & (n - 1) == 0 for n in (n_grp, n_shard))
        links = bits_of(n_grp) - 1 + bits_of(n_shard)
        matched = {link for stages, _ in REDUCE for stage in stages for link in stage} == set(range(links))
        if powers and n_grp > 2 and matched and cols == LANES * n_grp and rows % TILE == 0:
            return fused(mesh, grads, master, moment_one, moment_two, step_count)
        return plain(grads, master, moment_one, moment_two, step_count)

    return jax.shard_map(
        shards,
        mesh=mesh,
        in_specs=(
            P("grp", "shard", None, None),
            P("shard", None),
            P("shard", None),
            P("shard", None),
            P(),
        ),
        out_specs=(P("shard", None), P("shard", None), P("shard", None), P()),
        check_vma=False,
    )
```
